32 devices in a mesh: lon: 8 (over z, x), lat: 4 (over y, core).
Axes of the slice: x: 2, y: 2, z: 4, core: 2. Of those that a mesh axis runs over, the one named last changes fastest.
Arguments:
- tracers: float32 [40, 8, 32, 1024], P(None, None, 'lat', 'lon'), may hold values from -6 to 6
- kmt: int32 [32, 1024], P('lat', 'lon'), may hold values from 0 to 8
Outputs:
- updated: float32 [40, 8, 32, 1024], P(None, None, 'lat', 'lon')
The draws below stay inside these ranges and needn't reach their ends.
Inputs may be any that keep to these rules, and one draw needn't show every extreme that they name: Level k of column (j, i) is ocean exactly when k < kmt[j, i].
All inputs are finite; a program needn't handle non-finite values.
Results may differ from the reference program's by a relative error of at most 0.00002.
Values sent between devices are 32-bit elements; how exact they have to be, the bound alone decides.
No kernel may reach another device: no remote copies, remote signals or barrier semaphores. Data moves between devices by JAX's collectives and lax.ppermute only.
A program may use at most 64 MiB of HBM per device.

```python
import jax
import jax.numpy as jnp
from jax import lax

NTRAC = 40
NZ = 8
NY = 32
NX = 1024


def with_ends(array, rng, least, largest):
    longest = array.shape.index(max(array.shape))
    spots = []
    for shift in (0, 1):
        where = [jax.random.randint(jax.random.fold_in(rng, axis), (), 0, length) for axis, length in enumerate(array.shape)]
        where[longest] = (where[longest] + shift) % array.shape[longest]
        spots.append(tuple(where))
    return array.at[spots[0]].set(least).at[spots[1]].set(largest)


def block_scale(key, extent, pieces, least, largest):
    level, own = 1.0, jax.random.fold_in(key, 6)
    for dim, blocks in pieces:
        heights = jnp.exp(jax.random.uniform(jax.random.fold_in(own, dim), (blocks,), jnp.float32, least / len(pieces), largest / len(pieces)))
        level = level * jnp.repeat(heights, extent[dim] // blocks).reshape([-1 if axis == dim else 1 for axis in range(len(extent))])
    return level


def normal_values(rng, dims, scale, bound, pieces=(), kind=jnp.bfloat16):
    level = block_scale(rng, dims, pieces, -0.22, 0.18) if pieces else 1.0
    values = jax.random.normal(rng, dims, jnp.float32) * scale * level
    return jnp.minimum(jnp.maximum(values, -bound), bound).astype(kind)


def setup_inputs(seed: int = 0) -> dict:
    streams_of = jax.random.split(jax.random.key(seed), 3)
    tracers = normal_values(streams_of[0], (NTRAC, NZ, NY, NX), 1.0, 6.0, ((2, 4), (3, 8)), jnp.float32)
    kmt = with_ends(jax.random.randint(streams_of[1], (NY, NX), 0, NZ + 1), jax.random.fold_in(streams_of[1], 1), 0, NZ).astype(jnp.int32)
    return dict(tracers=tracers, kmt=kmt)


THERMAL = 0.2
HALINE = 0.8
REDI_COEF = 0.1
SKEW_COEF = 0.05
SLOPE_MAX = 0.6
SLOPE_WIDTH = 0.2


def taper(slope):
    return slope * 0.5 * (1.0 + jnp.tanh((SLOPE_MAX - jnp.abs(slope)) / SLOPE_WIDTH))


def pad_levels(values):
    zero_layer = jnp.zeros_like(values[..., :1, :, :])
    return jnp.concatenate([zero_layer, values, zero_layer], axis=-3)


def slope_fields(density, wet_mask):
    level_mask = wet_mask[1:] * wet_mask[:-1]
    strat = (density[1:] - density[:-1]) * level_mask
    strat_pad = pad_levels(strat)
    strat_cell = 0.5 * (strat_pad[:-1] + strat_pad[1:])
    east_mask = wet_mask[:, 1:-1, :-1] * wet_mask[:, 1:-1, 1:]
    north_mask = wet_mask[:, :-1, 1:-1] * wet_mask[:, 1:, 1:-1]
    grad_east = (density[:, 1:-1, 1:] - density[:, 1:-1, :-1]) * east_mask
    strat_east = 0.5 * (strat_cell[:, 1:-1, 1:] + strat_cell[:, 1:-1, :-1])
    slope_x = taper(grad_east / jnp.maximum(strat_east, 1.0))
    grad_north = (density[:, 1:, 1:-1] - density[:, :-1, 1:-1]) * north_mask
    strat_north = 0.5 * (strat_cell[:, 1:, 1:-1] + strat_cell[:, :-1, 1:-1])
    slope_y = taper(grad_north / jnp.maximum(strat_north, 1.0))
    cell_x = 0.5 * (slope_x[..., :-1] + slope_x[..., 1:])
    cell_y = 0.5 * (slope_y[:, :-1, :] + slope_y[:, 1:, :])
    level_x = 0.5 * (cell_x[:-1] + cell_x[1:])
    level_y = 0.5 * (cell_y[:-1] + cell_y[1:])
    return (level_mask, east_mask, north_mask, slope_x, slope_y, level_x, level_y)


def tracer_step(field, fields):
    level_mask, east_mask, north_mask, slope_x, slope_y, level_x, level_y = fields
    vert_diff = (field[..., 1:, :, :] - field[..., :-1, :, :]) * level_mask
    vert_pad = pad_levels(vert_diff)
    vert_cell = 0.5 * (vert_pad[..., :-1, :, :] + vert_pad[..., 1:, :, :])
    grad_x = (field[..., 1:-1, 1:] - field[..., 1:-1, :-1]) * east_mask
    grad_y = (field[..., 1:, 1:-1] - field[..., :-1, 1:-1]) * north_mask
    flux_x = -(REDI_COEF * grad_x + (REDI_COEF - SKEW_COEF) * slope_x
               * 0.5 * (vert_cell[..., 1:-1, 1:] + vert_cell[..., 1:-1, :-1])) * east_mask
    flux_y = -(REDI_COEF * grad_y + (REDI_COEF - SKEW_COEF) * slope_y
               * 0.5 * (vert_cell[..., 1:, 1:-1] + vert_cell[..., :-1, 1:-1])) * north_mask
    cell_gx = 0.5 * (grad_x[..., :-1] + grad_x[..., 1:])
    cell_gy = 0.5 * (grad_y[..., :-1, :] + grad_y[..., 1:, :])
    level_gx = 0.5 * (cell_gx[..., :-1, :, :] + cell_gx[..., 1:, :, :])
    level_gy = 0.5 * (cell_gy[..., :-1, :, :] + cell_gy[..., 1:, :, :])
    flux_z = -((REDI_COEF + SKEW_COEF) * (level_x * level_gx + level_y * level_gy)
               + REDI_COEF * (level_x * level_x + level_y * level_y) * vert_diff[..., 1:-1, 1:-1]) * level_mask[:, 1:-1, 1:-1]
    flux_pad = pad_levels(flux_z)
    tendency = -((flux_x[..., 1:] - flux_x[..., :-1]) + (flux_y[..., 1:, :] - flux_y[..., :-1, :])
                 + (flux_pad[..., 1:, :, :] - flux_pad[..., :-1, :, :]))
    return field[..., 1:-1, 1:-1] + tendency


def extend(field):
    beside_all = jnp.concatenate([field[..., -1:], field, field[..., :1]], axis=-1)
    north_row = beside_all[..., -1:, ::-1]
    south_row = jnp.zeros_like(beside_all[..., :1, :])
    return jnp.concatenate([south_row, beside_all, north_row], axis=-2)


def reference(tracers, kmt):
    level_index = lax.broadcasted_iota(jnp.int32, (NZ, NY, NX), 0)
    wet_mask = (level_index < kmt[None]).astype(jnp.float32)
    density = HALINE * tracers[1] - THERMAL * tracers[0]
    fields = slope_fields(extend(density), extend(wet_mask))
    return lax.map(lambda single: tracer_step(extend(single), fields), tracers)
```

```python
import functools

import jax
import jax.numpy as jnp
from jax import lax
from jax.experimental import pallas as pl
from jax.experimental.pallas import tpu as pltpu
from jax.sharding import PartitionSpec as P

THERMAL = 0.2
HALINE = 0.8
REDI = 0.1
SKEW = 0.05
SLOPE_MAX = 0.6
SLOPE_WIDTH = 0.2
FACE = 0.25 * (REDI - SKEW)
LEVEL = 0.25 * (REDI + SKEW) / REDI
CHUNKS = 5


def taper(slope):
    return slope * 0.5 * (1.0 + jnp.tanh((SLOPE_MAX - jnp.abs(slope)) * (1.0 / SLOPE_WIDTH)))


def lanes_of(shape):
    return lax.broadcasted_iota(jnp.int32, shape, len(shape) - 1)


def rows_of(shape):
    return lax.broadcasted_iota(jnp.int32, shape, len(shape) - 2)


def density_of(heat, salt):
    return HALINE * salt - THERMAL * heat


def as_mask(flag):
    return jnp.where(flag, 1.0, 0.0)


def slope_at(here, there, mask, strat_here, strat_there):
    return taper((here - there) * mask / jnp.maximum(0.5 * (strat_here + strat_there), 1.0))


def level_lists(values, masks):
    diffs = [(values[k + 1] - values[k]) * masks[k] for k in range(len(values) - 1)]
    sums = [diffs[0]] + [a + b for a, b in zip(diffs, diffs[1:])] + [diffs[-1]]
    return diffs, sums


def level_rows(values, mask):
    diffs = (pltpu.roll(values, values.shape[0] - 1, 0) - values) * mask
    return diffs, diffs + pltpu.roll(diffs, 1, 0)


def pack_kernel(dims, info, x_hbm, kmt_ref, x_ref, east_ref, west_ref, even_ref, odd_ref, sems):
    nt, nz, rows, cols, mirror_color = dims
    per = cols // nt
    step = nt // CHUNKS
    copies = []
    for c in range(CHUNKS):
        part = pl.ds(c * step * nz * rows, step * nz * rows)
        copies.append(pltpu.make_async_copy(x_hbm.at[part], x_ref.at[part], sems.at[c]))
        copies[-1].start()
    lane = lanes_of((rows, cols))
    odd, top = info[0] == 1, info[1] == 1
    kmt = kmt_ref[...].astype(jnp.float32)
    packs = nz // per + 1
    east, west = [jnp.zeros((rows, cols), jnp.float32)] * packs, [jnp.zeros((rows, cols), jnp.float32)] * packs
    spot = (nz % per) * nt
    last = (lane >= spot) & (lane < spot + nt)
    east[-1] = jnp.where(last, jnp.broadcast_to(kmt[:, cols - 1 :], (rows, cols)), 0.0)
    west[-1] = jnp.where(last, jnp.broadcast_to(kmt[:, :1], (rows, cols)), 0.0)

    def put_rows(low, high, start):
        count = low.shape[0]
        index = lanes_of((count, cols))
        turned = jnp.take_along_axis(high, jnp.where(top, cols - 1 - index, index), axis=1, mode="promise_in_bounds")
        refs = (even_ref, odd_ref)
        for color in (0, 1):
            up = turned if color == mirror_color else high
            goes_up = odd if color == 1 else jnp.logical_not(odd)
            refs[color][pl.ds(start, count), :] = jnp.where(goes_up, up, low)

    put_rows(jnp.broadcast_to(kmt[:1], (nz, cols)), jnp.broadcast_to(kmt[rows - 1 :], (nz, cols)), nt * nz)
    for c in range(CHUNKS):
        copies[c].wait()
        for t in range(c * step, (c + 1) * step):
            for k in range(nz):
                value = x_ref[pl.ds((t * nz + k) * rows, rows), :]
                spot = (k % per) * nt + t
                here = lane == spot
                east[k // per] = jnp.where(here, pltpu.roll(value, (spot + 1) % cols, 1), east[k // per])
                west[k // per] = jnp.where(here, pltpu.roll(value, spot, 1), west[k // per])
            low = x_ref[pl.ds(t * nz * rows, nz, stride=rows), :]
            high = x_ref[pl.ds(t * nz * rows + rows - 1, nz, stride=rows), :]
            put_rows(low, high, t * nz)
    for i in range(packs):
        east_ref[pl.ds(i * rows, rows), :] = east[i]
        west_ref[pl.ds(i * rows, rows), :] = west[i]


def main_kernel(dims, info, x_ref, kmt_ref, own_east, own_west, from_west, from_east, even_ref, odd_ref, out_hbm,
                out_ref, ax_ref, bx_ref, ay_ref, by_ref, wm_ref, p_ref, q_ref, z_ref, side_ref, sems):
    nt, nz, rows, cols, _ = dims
    per = cols // nt
    half = cols // 2
    shape = (rows, cols)
    lane, row = lanes_of(shape), rows_of(shape)
    odd, bottom = info[0] == 1, info[2] == 1
    kmt = kmt_ref[...].astype(jnp.float32)

    left = lane < half

    def pair(west, east, k):
        start = (k % per) * nt
        part = pl.ds((k // per) * rows, rows)
        return jnp.where(left, pltpu.roll(west[part, :], (cols - start) % cols, 1), pltpu.roll(east[part, :], (half - start) % cols, 1))

    def both(west, east):
        return jnp.where(left, jnp.broadcast_to(west, shape), jnp.broadcast_to(east, shape))

    own = [pair(own_west, own_east, k) for k in range(nz + 1)]
    ghost = [pair(from_west, from_east, k) for k in range(nz + 1)]
    own_kmt, ghost_kmt = own.pop(), ghost.pop()
    outward = jnp.where(left, -1.0, 1.0)
    own_wm = [as_mask(own_kmt > k + 1) for k in range(nz - 1)]
    ghost_wm = [as_mask(ghost_kmt > k + 1) for k in range(nz - 1)]
    side_mask = [as_mask(jnp.minimum(own_kmt, ghost_kmt) > k) for k in range(nz)]

    def side_density(values):
        return [density_of(v, pltpu.roll(v, cols - 1, 1)) for v in values]

    own_density, ghost_density = side_density(own), side_density(ghost)
    own_strat = level_lists(own_density, own_wm)[1]
    ghost_strat = level_lists(ghost_density, ghost_wm)[1]
    side_slope = []
    for k in range(nz):
        s = outward * slope_at(ghost_density[k], own_density[k], side_mask[k], 0.5 * own_strat[k], 0.5 * ghost_strat[k])
        side_slope.append(both(s[:, :1], s[:, half : half + 1]))

    flat = (nz, cols)
    depth = rows_of(flat)

    def ends(index):
        first, second = even_ref[pl.ds(index, nz), :], odd_ref[pl.ds(index, nz), :]
        return jnp.where(odd, first, second), jnp.where(odd, second, first)

    def own_rows(t):
        start = t * nz * rows
        return x_ref[pl.ds(start, nz, stride=rows), :], x_ref[pl.ds(start + rows - 1, nz, stride=rows), :]

    south_kmt, north_kmt = ends(nt * nz)
    south_kmt = jnp.where(bottom, 0.0, south_kmt)
    low_kmt, high_kmt = jnp.broadcast_to(kmt[:1], flat), jnp.broadcast_to(kmt[rows - 1 :], flat)
    level = depth.astype(jnp.float32)

    def end_slope(kmts, heats, salts):
        masks = [as_mask(k > level + 1.0) for k in kmts]
        mask = as_mask(jnp.minimum(*kmts) > level)
        densities = [density_of(h, s) for h, s in zip(heats, salts)]
        strats = [0.5 * level_rows(d, m)[1] for d, m in zip(densities, masks)]
        return masks, mask, slope_at(densities[1], densities[0], mask, *strats)

    heat_ends, salt_ends, heat_own, salt_own = ends(0), ends(nz), own_rows(0), own_rows(1)
    south_wms, south_mask, south_slope = end_slope((south_kmt, low_kmt), (heat_ends[0], heat_own[0]), (salt_ends[0], salt_own[0]))
    north_wms, north_mask, north_slope = end_slope((high_kmt, north_kmt), (heat_own[1], heat_ends[1]), (salt_own[1], salt_ends[1]))

    heat = [x_ref[pl.ds(k * rows, rows), :] for k in range(nz)]
    salt = [x_ref[pl.ds((nz + k) * rows, rows), :] for k in range(nz)]
    density = [density_of(h, s) for h, s in zip(heat, salt)]
    wm = [as_mask(kmt > k + 1) for k in range(nz - 1)]
    strat = [0.5 * s for s in level_lists(density, wm)[1]]
    kmt_x = jnp.minimum(kmt, pltpu.roll(kmt, 1, 1))
    kmt_y = jnp.minimum(kmt, pltpu.roll(kmt, 1, 0))
    sum_x, sum_y = [], []
    for k in range(nz):
        part = pl.ds(k * rows, rows)
        mask = as_mask(kmt_x > k)
        slope = slope_at(density[k], pltpu.roll(density[k], 1, 1), mask, strat[k], pltpu.roll(strat[k], 1, 1))
        ax_ref[part, :] = jnp.where(lane == 0, 0.0, REDI * mask)
        bx_ref[part, :] = jnp.where(lane == 0, 0.0, FACE * slope)
        slope = jnp.where(lane == 0, side_slope[k], slope)
        sum_x.append(slope + jnp.where(lane == cols - 1, side_slope[k], pltpu.roll(slope, cols - 1, 1)))
        mask = as_mask(kmt_y > k)
        slope = slope_at(density[k], pltpu.roll(density[k], 1, 0), mask, strat[k], pltpu.roll(strat[k], 1, 0))
        ay_ref[part, :] = jnp.where(row == 0, 0.0, REDI * mask)
        by_ref[part, :] = jnp.where(row == 0, 0.0, FACE * slope)
        slope = jnp.where(row == 0, jnp.broadcast_to(south_slope[k : k + 1], shape), slope)
        sum_y.append(slope + jnp.where(row == rows - 1, jnp.broadcast_to(north_slope[k : k + 1], shape), pltpu.roll(slope, rows - 1, 0)))
    side_p = []
    for k in range(nz - 1):
        part = pl.ds(k * rows, rows)
        level_x = 0.25 * (sum_x[k] + sum_x[k + 1])
        level_y = 0.25 * (sum_y[k] + sum_y[k + 1])
        p = LEVEL * level_x * wm[k]
        wm_ref[part, :] = wm[k]
        p_ref[part, :] = p
        q_ref[part, :] = LEVEL * level_y * wm[k]
        z_ref[part, :] = REDI * (level_x * level_x + level_y * level_y) * wm[k]
        side_p.append(both(p[:, :1], p[:, cols - 1 :]))
    q_ref[pl.ds((nz - 1) * rows, rows), :] = jnp.zeros(shape, jnp.float32)

    own_sum, ghost_sum = level_lists(own, own_wm)[1], level_lists(ghost, ghost_wm)[1]
    grad = [REDI * side_mask[k] * (ghost[k] - own[k]) for k in range(nz)]
    flux = [grad[k] + outward * FACE * side_slope[k] * (own_sum[k] + ghost_sum[k]) for k in range(nz)]
    tilt = [side_p[k] * outward * (grad[k] + grad[k + 1]) for k in range(nz - 1)]
    turn = lax.rem(lane + 1, cols)
    index = jnp.where(lax.rem(lane, 2) == 0, lane // 2, half + turn // 2)
    for k in range(nz):
        added = flux[k]
        if k < nz - 1:
            added = added + tilt[k]
        if k > 0:
            added = added - tilt[k - 1]
        side_ref[pl.ds(k * rows, rows), :] = jnp.take_along_axis(added, index, axis=1, mode="promise_in_bounds")

    end_coefs = []
    for wms, mask, slope, first in ((south_wms, south_mask, south_slope, 0), (north_wms, north_mask, north_slope, rows - 1)):
        end_coefs.append((wms, REDI * mask, FACE * slope, q_ref[pl.ds(first, nz, stride=rows), :]))
    outer = (lane == 0) | (lane == cols - 1)

    def cell_step(t, carry):
        def load(ref, k):
            return ref[pl.ds(k * rows, rows), :]

        base = t * (nz * rows)
        value = [x_ref[pl.ds(pl.multiple_of(base + k * rows, rows), rows), :] for k in range(nz)]
        diff, total = level_lists(value, [load(wm_ref, k) for k in range(nz - 1)])
        shift = lax.rem(cols - 2 * t, cols)
        new, cell_x, cell_y = [], [], []
        for k in range(nz):
            grad = load(ax_ref, k) * (value[k] - pltpu.roll(value[k], 1, 1))
            flux = grad + load(bx_ref, k) * (total[k] + pltpu.roll(total[k], 1, 1))
            cell_x.append(grad + pltpu.roll(grad, cols - 1, 1))
            gain = pltpu.roll(flux, cols - 1, 1) - flux
            grad = load(ay_ref, k) * (value[k] - pltpu.roll(value[k], 1, 0))
            flux = grad + load(by_ref, k) * (total[k] + pltpu.roll(total[k], 1, 0))
            cell_y.append(grad + pltpu.roll(grad, rows - 1, 0))
            gain = gain + (pltpu.roll(flux, rows - 1, 0) - flux)
            gain = gain + jnp.where(outer, pltpu.roll(load(side_ref, k), shift, 1), 0.0)
            new.append(value[k] + gain)
        down = None
        for k in range(nz):
            result = new[k]
            if k > 0:
                result = result - down
            if k < nz - 1:
                down = (load(p_ref, k) * (cell_x[k] + cell_x[k + 1]) + load(q_ref, k) * (cell_y[k] + cell_y[k + 1])
                        + load(z_ref, k) * diff[k])
                result = result + down
            out_ref[pl.ds(pl.multiple_of(base + k * rows, rows), rows), :] = result
        return carry

    def end_step(t):
        for end in (0, 1):
            wms, a, b, q = end_coefs[end]
            here, there = own_rows(t)[end], ends(t * nz)[end]
            below, above = (there, here) if end == 0 else (here, there)
            sums = level_rows(below, wms[0])[1] + level_rows(above, wms[1])[1]
            grad = a * (above - below)
            flux = grad + b * sums
            tilt = q * (grad + pltpu.roll(grad, nz - 1, 0))
            gain = flux if end == 1 else -flux
            part = pl.ds(t * nz * rows + (rows - 1 if end else 0), nz, stride=rows)
            out_ref[part, :] = out_ref[part, :] + (gain + (tilt - pltpu.roll(tilt, 1, 0)))

    step = nt // CHUNKS
    copies = []
    for c in range(CHUNKS):
        lax.fori_loop(c * step, (c + 1) * step, cell_step, 0)
        for t in range(c * step, (c + 1) * step):
            end_step(t)
        part = pl.ds(c * step * nz * rows, step * nz * rows)
        copies.append(pltpu.make_async_copy(out_ref.at[part], out_hbm.at[part], sems.at[c]))
        copies[-1].start()
    for copy in copies:
        copy.wait()


def row_pairs(color, lons, lats):
    pairs = []
    for lon in range(lons):
        for lat in range(lats - 1):
            if lat % 2 == color:
                pairs += [(lon * lats + lat, lon * lats + lat + 1), (lon * lats + lat + 1, lon * lats + lat)]
        if (lats - 1) % 2 == color:
            pairs.append((lon * lats + lats - 1, (lons - 1 - lon) * lats + lats - 1))
    free_in = sorted(set(range(lons * lats)) - {b for _, b in pairs})
    free_out = set(range(lons * lats)) - {a for a, _ in pairs}
    for target in free_in:
        lon, lat = divmod(target, lats)
        source = (lon ^ 1 if lons % 2 == 0 else (lon + 1) % lons) * lats + lat
        assert source in free_out
        pairs.append((source, target))
    return pairs


def local(tracers, kmt):
    nt, nz, rows, cols = tracers.shape
    lons, lats = lax.axis_size("lon"), lax.axis_size("lat")
    dims = (nt, nz, rows, cols, (lats - 1) % 2)
    per = cols // nt
    packed = ((nz // per + 1) * rows, cols)
    edge = (nt * nz + nz, cols)
    lat = lax.axis_index("lat")
    info = jnp.stack([lat % 2, (lat == lats - 1).astype(jnp.int32), (lat == 0).astype(jnp.int32)])
    vmem = pl.BlockSpec(memory_space=pltpu.VMEM)
    smem = pl.BlockSpec(memory_space=pltpu.SMEM)
    anywhere = pl.BlockSpec(memory_space=pl.ANY)
    x = tracers.reshape(nt * nz * rows, cols)
    x_near, east, west, even, odd = pl.pallas_call(
        functools.partial(pack_kernel, dims),
        out_shape=[pltpu.VMEM(s, jnp.float32) for s in (x.shape, packed, packed, edge, edge)],
        in_specs=[smem, anywhere, vmem],
        out_specs=[vmem] * 5,
        scratch_shapes=[pltpu.SemaphoreType.DMA((CHUNKS,))],
        name="pack",
    )(info, x, kmt)
    ring = [(i, (i + 1) % lons) for i in range(lons)]
    from_west = lax.ppermute(east, "lon", ring)
    from_odd = lax.ppermute(odd, ("lon", "lat"), row_pairs(1, lons, lats))
    from_even = lax.ppermute(even, ("lon", "lat"), row_pairs(0, lons, lats))
    from_east = lax.ppermute(west, "lon", [(b, a) for a, b in ring])
    cells = lambda levels: pltpu.VMEM((levels * rows, cols), jnp.float32)
    out = pl.pallas_call(
        functools.partial(main_kernel, dims),
        out_shape=jax.ShapeDtypeStruct(x.shape, jnp.float32),
        in_specs=[smem] + [vmem] * 8,
        out_specs=anywhere,
        scratch_shapes=[pltpu.VMEM(x.shape, jnp.float32)] + [cells(nz)] * 4 + [cells(nz - 1)] * 2 + [cells(nz), cells(nz - 1), cells(nz)]
        + [pltpu.SemaphoreType.DMA((CHUNKS,))],
        name="step",
    )(info, x_near, kmt, east, west, from_west, from_east, from_even, from_odd)
    return out.reshape(tracers.shape)


def solution(mesh):
    return jax.shard_map(
        local,
        mesh=mesh,
        in_specs=(P(None, None, "lat", "lon"), P("lat", "lon")),
        out_specs=P(None, None, "lat", "lon"),
        check_vma=False,
    )
```

```python
import functools

import jax
import jax.numpy as jnp
from jax import lax
from jax.experimental import pallas as pl
from jax.experimental.pallas import tpu as pltpu
from jax.sharding import PartitionSpec as P

THERMAL = 0.2
HALINE = 0.8
REDI = 0.1
SKEW = 0.05
SLOPE_MAX = 0.6
SLOPE_WIDTH = 0.2
FACE = 0.25 * (REDI - SKEW)
LEVEL = 0.25 * (REDI + SKEW) / REDI
CHUNKS = 5
UNROLL = 8


def taper(slope):
    return slope * 0.5 * (1.0 + jnp.tanh((SLOPE_MAX - jnp.abs(slope)) * (1.0 / SLOPE_WIDTH)))


def lanes_of(shape):
    return lax.broadcasted_iota(jnp.int32, shape, len(shape) - 1)


def rows_of(shape):
    return lax.broadcasted_iota(jnp.int32, shape, len(shape) - 2)


def density_of(heat, salt):
    return HALINE * salt - THERMAL * heat


def as_mask(flag):
    return jnp.where(flag, 1.0, 0.0)


def slope_at(here, there, mask, strat_here, strat_there):
    return taper((here - there) * mask / jnp.maximum(0.5 * (strat_here + strat_there), 1.0))


def level_lists(values, masks):
    diffs = [(values[k + 1] - values[k]) * masks[k] for k in range(len(values) - 1)]
    sums = [diffs[0]] + [a + b for a, b in zip(diffs, diffs[1:])] + [diffs[-1]]
    return diffs, sums


def level_rows(values, mask):
    diffs = (pltpu.roll(values, values.shape[0] - 1, 0) - values) * mask
    return diffs, diffs + pltpu.roll(diffs, 1, 0)


def position():
    lat = lax.axis_index("lat")
    return lax.rem(lat, 2) == 1, lat == 0, lat == lax.axis_size("lat") - 1


def pick(values, index):
    return jnp.take_along_axis(values, index, axis=1, mode="promise_in_bounds")


def pair_of(west, east, cols=128):
    shape = (west.shape[0], cols)
    return jnp.where(lax.rem(lanes_of(shape), 2) == 0, jnp.broadcast_to(west, shape), jnp.broadcast_to(east, shape))


def pack_kernel(dims, x_hbm, kmt_hbm, x_ref, own_ref, east_ref, west_ref, even_ref, odd_ref, kmt_ref, raw_ref, sems):
    nt, nz, rows, cols, mirror_color = dims
    per = cols // nt
    step = nt // CHUNKS
    copies = []
    for c in range(CHUNKS):
        part = pl.ds(c * step * nz * rows, step * nz * rows)
        copies.append(pltpu.make_async_copy(x_hbm.at[part], x_ref.at[part], sems.at[c]))
        copies[-1].start()
    kmt_copy = pltpu.make_async_copy(kmt_hbm, raw_ref, sems.at[CHUNKS])
    kmt_copy.start()
    shape = (rows, cols)
    lane = lanes_of(shape)
    odd, _, top = position()

    def put_rows(low, high, start):
        index = lanes_of(low.shape)
        turned = pick(high, jnp.where(top, cols - 1 - index, index))
        for color, ref in ((0, even_ref), (1, odd_ref)):
            up = turned if color == mirror_color else high
            goes_up = odd if color == 1 else jnp.logical_not(odd)
            ref[pl.ds(start, nz), :] = jnp.where(goes_up, up, low)

    pairs = [jnp.zeros(shape, jnp.float32)] * nz
    for c in range(CHUNKS):
        copies[c].wait()
        for t in range(c * step, (c + 1) * step):
            here = (lane == 2 * t) | (lane == (2 * t - 1) % cols)
            for k in range(nz):
                value = x_ref[pl.ds((t * nz + k) * rows, rows), :]
                pairs[k] = jnp.where(here, pltpu.roll(value, 2 * t, 1) if t else value, pairs[k])
    kmt_copy.wait()
    kmt = raw_ref[...].astype(jnp.float32)
    kmt_ref[...] = kmt
    for k in range(nz):
        own_ref[pl.ds(k * rows, rows), :] = pairs[k]
    for j in range(nz // per + 1):
        east = west = jnp.zeros(shape, jnp.float32)
        for i in range(per):
            k, start = j * per + i, i * nt
            if k > nz:
                break
            index = lax.rem(2 * (lane - start + cols), cols)
            if k == nz:
                side = (jnp.broadcast_to(kmt[:, cols - 1 :], shape), jnp.broadcast_to(kmt[:, :1], shape))
            else:
                side = pick(pairs[k], lax.rem(index + cols - 1, cols)), pick(pairs[k], index)
            east, west = (jnp.where(lane >= start, a, b) for a, b in zip(side, (east, west)))
        east_ref[pl.ds(j * rows, rows), :] = east
        west_ref[pl.ds(j * rows, rows), :] = west
    for t in range(nt):
        start = t * nz * rows
        put_rows(x_ref[pl.ds(start, nz, stride=rows), :], x_ref[pl.ds(start + rows - 1, nz, stride=rows), :], t * nz)
    put_rows(jnp.broadcast_to(kmt[:1], (nz, cols)), jnp.broadcast_to(kmt[rows - 1 :], (nz, cols)), nt * nz)


def inner_kernel(dims, x_ref, kmt_ref, base_ref, cx_ref, cy_ref, diff_ref, sum_x_ref, sum_y_ref, inner_ref,
                 ax_ref, bx_ref, ay_ref, by_ref):
    nt, nz, rows, cols, _ = dims
    shape = (rows, cols)
    lane, row = lanes_of(shape), rows_of(shape)
    kmt = kmt_ref[...]
    heat = [x_ref[pl.ds(k * rows, rows), :] for k in range(nz)]
    salt = [x_ref[pl.ds((nz + k) * rows, rows), :] for k in range(nz)]
    density = [density_of(h, s) for h, s in zip(heat, salt)]
    wm = [as_mask(kmt > k + 1) for k in range(nz - 1)]
    kmt_w = pltpu.roll(kmt, 1, 1)
    wm_w = [as_mask(kmt_w > k + 1) for k in range(nz - 1)]
    strat = [0.5 * s for s in level_lists(density, wm)[1]]
    kmt_x = jnp.where(lane == 0, 0.0, jnp.minimum(kmt, kmt_w))
    kmt_y = jnp.where(row == 0, 0.0, jnp.minimum(kmt, pltpu.roll(kmt, 1, 0)))
    for k in range(nz):
        part = pl.ds(k * rows, rows)
        mask = as_mask(kmt_x > k)
        slope = slope_at(density[k], pltpu.roll(density[k], 1, 1), mask, strat[k], pltpu.roll(strat[k], 1, 1))
        ax_ref[part, :] = REDI * mask
        bx_ref[part, :] = FACE * slope
        sum_x_ref[part, :] = slope + pltpu.roll(slope, cols - 1, 1)
        inner_ref[part, :] = pair_of(slope[:, 1:2], slope[:, cols - 1 :])
        mask = as_mask(kmt_y > k)
        slope = slope_at(density[k], pltpu.roll(density[k], 1, 0), mask, strat[k], pltpu.roll(strat[k], 1, 0))
        ay_ref[part, :] = REDI * mask
        by_ref[part, :] = FACE * slope
        sum_y_ref[part, :] = slope + pltpu.roll(slope, rows - 1, 0)

    def load(ref, k):
        return ref[pl.ds(k * rows, rows), :]

    def tracer(t):
        base = t * (nz * rows)
        part = lambda k: pl.ds(pl.multiple_of(base + k * rows, rows), rows)
        value = [x_ref[part(k), :] for k in range(nz)]
        beside = [pltpu.roll(v, 1, 1) for v in value]
        diff, total = level_lists(value, wm)
        total_w = level_lists(beside, wm_w)[1]
        cell_x, cell_y = [], []
        for k in range(nz):
            grad = load(ax_ref, k) * (value[k] - beside[k])
            flux = grad + load(bx_ref, k) * (total[k] + total_w[k])
            cell_x.append(grad + pltpu.roll(grad, cols - 1, 1))
            gain = pltpu.roll(flux, cols - 1, 1) - flux
            grad = load(ay_ref, k) * (value[k] - pltpu.roll(value[k], 1, 0))
            flux = grad + load(by_ref, k) * (total[k] + pltpu.roll(total[k], 1, 0))
            cell_y.append(grad + pltpu.roll(grad, rows - 1, 0))
            base_ref[part(k), :] = value[k] + (gain + (pltpu.roll(flux, rows - 1, 0) - flux))
        for k in range(nz - 1):
            cx_ref[part(k), :] = cell_x[k] + cell_x[k + 1]
            cy_ref[part(k), :] = cell_y[k] + cell_y[k + 1]
            diff_ref[part(k), :] = diff[k]

    def block(i, carry):
        for t in range(UNROLL):
            tracer(i * UNROLL + t)
        return carry

    lax.fori_loop(0, nt // UNROLL, block, 0)


def outer_kernel(dims, x_ref, kmt_ref, own_ref, base_ref, cx_ref, cy_ref, diff_ref, sum_x_ref, sum_y_ref, inner_ref,
                 from_west, from_east, even_ref, odd_ref, out_hbm, out_ref, p_ref, q_ref, z_ref, side_ref, sems):
    nt, nz, rows, cols, _ = dims
    per = cols // nt
    shape = (rows, cols)
    lane, row = lanes_of(shape), rows_of(shape)
    odd, bottom, _ = position()
    kmt = kmt_ref[...]

    def load(ref, k):
        return ref[pl.ds(k * rows, rows), :]

    even_lane = lax.rem(lane, 2) == 0
    slot = jnp.where(even_lane, lane // 2, lax.rem(lane + 1, cols) // 2)
    outward = jnp.where(even_lane, -1.0, 1.0)

    def ghost_at(k):
        index = lax.rem(slot + (k % per) * nt, cols)
        return jnp.where(even_lane, pick(load(from_west, k // per), index), pick(load(from_east, k // per), index))

    own = [load(own_ref, k) for k in range(nz)]
    ghost = [ghost_at(k) for k in range(nz + 1)]
    own_kmt, ghost_kmt = pair_of(kmt[:, :1], kmt[:, cols - 1 :]), ghost.pop()
    own_wm = [as_mask(own_kmt > k + 1) for k in range(nz - 1)]
    ghost_wm = [as_mask(ghost_kmt > k + 1) for k in range(nz - 1)]
    side_mask = [as_mask(jnp.minimum(own_kmt, ghost_kmt) > k) for k in range(nz)]

    def side_density(values):
        return [density_of(v, pltpu.roll(v, cols - 2, 1)) for v in values]

    own_density, ghost_density = side_density(own), side_density(ghost)
    own_strat = level_lists(own_density, own_wm)[1]
    ghost_strat = level_lists(ghost_density, ghost_wm)[1]
    first = [
        outward * slope_at(ghost_density[k], own_density[k], side_mask[k], 0.5 * own_strat[k], 0.5 * ghost_strat[k])
        for k in range(nz)
    ]
    side_slope = [pair_of(s[:, :1], s[:, cols - 1 :]) for s in first]
    outer = (lane == 0) | (lane == cols - 1)
    sum_x = [load(sum_x_ref, k) + jnp.where(outer, first[k], 0.0) for k in range(nz)]

    flat = (nz, cols)
    level = rows_of(flat).astype(jnp.float32)

    def ends(index):
        a, b = even_ref[pl.ds(index, nz), :], odd_ref[pl.ds(index, nz), :]
        return jnp.where(odd, a, b), jnp.where(odd, b, a)

    def own_rows(t):
        start = t * nz * rows
        return x_ref[pl.ds(start, nz, stride=rows), :], x_ref[pl.ds(start + rows - 1, nz, stride=rows), :]

    south_kmt, north_kmt = ends(nt * nz)
    south_kmt = jnp.where(bottom, 0.0, south_kmt)
    low_kmt, high_kmt = jnp.broadcast_to(kmt[:1], flat), jnp.broadcast_to(kmt[rows - 1 :], flat)

    def end_slope(kmts, heats, salts):
        masks = [as_mask(k > level + 1.0) for k in kmts]
        mask = as_mask(jnp.minimum(*kmts) > level)
        densities = [density_of(h, s) for h, s in zip(heats, salts)]
        strats = [0.5 * level_rows(d, m)[1] for d, m in zip(densities, masks)]
        return masks, mask, slope_at(densities[1], densities[0], mask, *strats)

    heat_ends, salt_ends, heat_own, salt_own = ends(0), ends(nz), own_rows(0), own_rows(1)
    south = end_slope((south_kmt, low_kmt), (heat_ends[0], heat_own[0]), (salt_ends[0], salt_own[0]))
    north = end_slope((high_kmt, north_kmt), (heat_own[1], heat_ends[1]), (salt_own[1], salt_ends[1]))
    sum_y = []
    for k in range(nz):
        below, above = jnp.broadcast_to(south[2][k : k + 1], shape), jnp.broadcast_to(north[2][k : k + 1], shape)
        sum_y.append(load(sum_y_ref, k) + jnp.where(row == 0, below, jnp.where(row == rows - 1, above, 0.0)))

    for k in range(nz - 1):
        part = pl.ds(k * rows, rows)
        wm = as_mask(kmt > k + 1)
        level_x, level_y = 0.25 * (sum_x[k] + sum_x[k + 1]), 0.25 * (sum_y[k] + sum_y[k + 1])
        p_ref[part, :] = LEVEL * level_x * wm
        q_ref[part, :] = LEVEL * level_y * wm
        z_ref[part, :] = REDI * (level_x * level_x + level_y * level_y) * wm
    q_ref[pl.ds((nz - 1) * rows, rows), :] = jnp.zeros(shape, jnp.float32)

    own_sum, ghost_sum = level_lists(own, own_wm)[1], level_lists(ghost, ghost_wm)[1]
    grad = [REDI * side_mask[k] * (ghost[k] - own[k]) for k in range(nz)]
    flux = [grad[k] + outward * FACE * side_slope[k] * (own_sum[k] + ghost_sum[k]) for k in range(nz)]
    both = [side_slope[k] + load(inner_ref, k) for k in range(nz)]
    tilt = [0.25 * LEVEL * (both[k] + both[k + 1]) * own_wm[k] * outward * (grad[k] + grad[k + 1]) for k in range(nz - 1)]
    for k in range(nz):
        added = flux[k]
        if k < nz - 1:
            added = added + tilt[k]
        if k > 0:
            added = added - tilt[k - 1]
        side_ref[pl.ds(k * rows, rows), :] = added

    end_coefs = []
    for (wms, mask, slope), start in ((south, 0), (north, rows - 1)):
        end_coefs.append((wms, REDI * mask, FACE * slope, q_ref[pl.ds(start, nz, stride=rows), :]))

    def cell_step(t):
        base = t * nz * rows
        part = lambda k: pl.ds(base + k * rows, rows)
        down = None
        for k in range(nz):
            side = load(side_ref, k)
            side = pltpu.roll(side, cols - 2 * t, 1) if t else side
            result = base_ref[part(k), :] + jnp.where(outer, side, 0.0)
            if k > 0:
                result = result - down
            if k < nz - 1:
                down = load(p_ref, k) * cx_ref[part(k), :] + load(q_ref, k) * cy_ref[part(k), :] + load(z_ref, k) * diff_ref[part(k), :]
                result = result + down
            out_ref[part(k), :] = result

    def end_step(t):
        for end in (0, 1):
            wms, a, b, q = end_coefs[end]
            here, there = own_rows(t)[end], ends(t * nz)[end]
            below, above = (there, here) if end == 0 else (here, there)
            sums = level_rows(below, wms[0])[1] + level_rows(above, wms[1])[1]
            grad = a * (above - below)
            flux = grad + b * sums
            tilt = q * (grad + pltpu.roll(grad, nz - 1, 0))
            gain = flux if end == 1 else -flux
            part = pl.ds(t * nz * rows + (rows - 1 if end else 0), nz, stride=rows)
            out_ref[part, :] = out_ref[part, :] + (gain + (tilt - pltpu.roll(tilt, 1, 0)))

    step = nt // CHUNKS
    copies = []
    for c in range(CHUNKS):
        for t in range(c * step, (c + 1) * step):
            cell_step(t)
        for t in range(c * step, (c + 1) * step):
            end_step(t)
        part = pl.ds(c * step * nz * rows, step * nz * rows)
        copies.append(pltpu.make_async_copy(out_ref.at[part], out_hbm.at[part], sems.at[c]))
        copies[-1].start()
    for copy in copies:
        copy.wait()


def row_pairs(color, lons, lats):
    pairs = []
    for lon in range(lons):
        for lat in range(lats - 1):
            if lat % 2 == color:
                pairs += [(lon * lats + lat, lon * lats + lat + 1), (lon * lats + lat + 1, lon * lats + lat)]
        if (lats - 1) % 2 == color:
            pairs.append((lon * lats + lats - 1, (lons - 1 - lon) * lats + lats - 1))
    free_in = sorted(set(range(lons * lats)) - {b for _, b in pairs})
    free_out = set(range(lons * lats)) - {a for a, _ in pairs}
    for target in free_in:
        lon, lat = divmod(target, lats)
        source = (lon ^ 1 if lons % 2 == 0 else (lon + 1) % lons) * lats + lat
        assert source in free_out
        pairs.append((source, target))
    return pairs


def local(tracers, kmt):
    nt, nz, rows, cols = tracers.shape
    lons, lats = lax.axis_size("lon"), lax.axis_size("lat")
    dims = (nt, nz, rows, cols, (lats - 1) % 2)
    packed = ((nz // (cols // nt) + 1) * rows, cols)
    edge = (nt * nz + nz, cols)
    level, block = (nz * rows, cols), (nt * nz * rows, cols)
    vmem, anywhere = pl.BlockSpec(memory_space=pltpu.VMEM), pl.BlockSpec(memory_space=pl.ANY)

    def call(kernel, inputs, out_shape, scratch, flops, specs=None):
        out = [pltpu.VMEM(s, jnp.float32) for s in out_shape] if specs is None else out_shape
        if specs is None:
            specs = [vmem] * len(out_shape)
        near = [a if a is x or a is kmt else pltpu.with_memory_space_constraint(a, pltpu.VMEM) for a in inputs]
        return pl.pallas_call(
            functools.partial(kernel, dims),
            out_shape=out,
            in_specs=[anywhere if a is x or a is kmt else vmem for a in inputs],
            out_specs=specs,
            scratch_shapes=scratch,
            cost_estimate=pl.CostEstimate(flops=flops, bytes_accessed=flops, transcendentals=0),
            compiler_params=pltpu.CompilerParams(vmem_limit_bytes=16 * 2**20),
        )(*near)

    x = tracers.reshape(block)
    cells = lambda levels: pltpu.VMEM((levels * rows, cols), jnp.float32)
    near, own, east, west, even, odd, near_kmt = call(
        pack_kernel,
        (x, kmt),
        (block, level, packed, packed, edge, edge, (rows, cols)),
        [pltpu.VMEM((rows, cols), jnp.int32), pltpu.SemaphoreType.DMA((CHUNKS + 1,))],
        1000000,
    )
    ring = [(i, (i + 1) % lons) for i in range(lons)]
    from_west = lax.ppermute(east, "lon", ring)
    from_odd = lax.ppermute(odd, ("lon", "lat"), row_pairs(1, lons, lats))
    from_even = lax.ppermute(even, ("lon", "lat"), row_pairs(0, lons, lats))
    from_east = lax.ppermute(west, "lon", [(b, a) for a, b in ring])
    inner = call(inner_kernel, (near, near_kmt), (block,) * 4 + (level,) * 3, [cells(nz)] * 4, 10000000)
    out = call(
        outer_kernel,
        (near, near_kmt, own, *inner, from_west, from_east, from_even, from_odd),
        jax.ShapeDtypeStruct(block, jnp.float32),
        [pltpu.VMEM(block, jnp.float32), cells(nz - 1), cells(nz), cells(nz - 1), cells(nz), pltpu.SemaphoreType.DMA((CHUNKS,))],
        10000000,
        anywhere,
    )
    return out.reshape(tracers.shape)


def solution(mesh):
    return jax.shard_map(
        local,
        mesh=mesh,
        in_specs=(P(None, None, "lat", "lon"), P("lat", "lon")),
        out_specs=P(None, None, "lat", "lon"),
        check_vma=False,
    )
```

```python
import functools

import jax
import jax.numpy as jnp
from jax import lax
from jax.experimental import pallas as pl
from jax.experimental.pallas import tpu as pltpu
from jax.sharding import PartitionSpec as P

THERMAL = 0.2
HALINE = 0.8
REDI = 0.1
SKEW = 0.05
SLOPE_MAX = 0.6
SLOPE_WIDTH = 0.2
FACE = 0.25 * (REDI - SKEW)
LEVEL = 0.25 * (REDI + SKEW) / REDI
CHUNKS = 5
UNROLL = 4
EARLY = 5


def taper(slope):
    return slope * 0.5 * (1.0 + jnp.tanh((SLOPE_MAX - jnp.abs(slope)) * (1.0 / SLOPE_WIDTH)))


def lanes_of(shape):
    return lax.broadcasted_iota(jnp.int32, shape, len(shape) - 1)


def rows_of(shape):
    return lax.broadcasted_iota(jnp.int32, shape, len(shape) - 2)


def density_of(heat, salt):
    return HALINE * salt - THERMAL * heat


def as_mask(flag):
    return jnp.where(flag, 1.0, 0.0)


def slope_at(here, there, mask, strat_here, strat_there):
    return taper((here - there) * mask / jnp.maximum(0.5 * (strat_here + strat_there), 1.0))


def level_lists(values, masks):
    diffs = [(values[k + 1] - values[k]) * masks[k] for k in range(len(values) - 1)]
    sums = [diffs[0]] + [a + b for a, b in zip(diffs, diffs[1:])] + [diffs[-1]]
    return diffs, sums


def level_rows(values, mask):
    diffs = (pltpu.roll(values, values.shape[0] - 1, 0) - values) * mask
    return diffs, diffs + pltpu.roll(diffs, 1, 0)


def position():
    lat = lax.axis_index("lat")
    return lax.rem(lat, 2) == 1, lat == 0, lat == lax.axis_size("lat") - 1


def pick(values, index):
    return jnp.take_along_axis(values, index, axis=1, mode="promise_in_bounds")


def pair_of(west, east, cols=128):
    shape = (west.shape[0], cols)
    return jnp.where(lax.rem(lanes_of(shape), 2) == 0, jnp.broadcast_to(west, shape), jnp.broadcast_to(east, shape))


def pack_kernel(dims, x_hbm, kmt_hbm, x_ref, own_ref, east_ref, west_ref, even_ref, odd_ref, kmt_ref, raw_ref, sems):
    nt, nz, rows, cols, mirror_color = dims
    per = cols // nt
    step = nt // CHUNKS
    copies = []
    for c in range(CHUNKS):
        part = pl.ds(c * step * nz * rows, step * nz * rows)
        copies.append(pltpu.make_async_copy(x_hbm.at[part], x_ref.at[part], sems.at[c]))
        copies[-1].start()
    kmt_copy = pltpu.make_async_copy(kmt_hbm, raw_ref, sems.at[CHUNKS])
    kmt_copy.start()
    shape = (rows, cols)
    lane = lanes_of(shape)
    odd, _, top = position()

    def put_rows(low, high, start):
        index = lanes_of(low.shape)
        turned = pick(high, jnp.where(top, cols - 1 - index, index))
        for color, ref in ((0, even_ref), (1, odd_ref)):
            up = turned if color == mirror_color else high
            goes_up = odd if color == 1 else jnp.logical_not(odd)
            ref[pl.ds(start, nz), :] = jnp.where(goes_up, up, low)

    pairs = [jnp.zeros(shape, jnp.float32)] * nz
    for c in range(CHUNKS):
        copies[c].wait()
        for t in range(c * step, (c + 1) * step):
            here = (lane == 2 * t) | (lane == (2 * t - 1) % cols)
            for k in range(nz):
                value = x_ref[pl.ds((t * nz + k) * rows, rows), :]
                pairs[k] = jnp.where(here, pltpu.roll(value, 2 * t, 1) if t else value, pairs[k])
    kmt_copy.wait()
    kmt = raw_ref[...].astype(jnp.float32)
    kmt_ref[...] = kmt
    for k in range(nz):
        own_ref[pl.ds(k * rows, rows), :] = pairs[k]
    for j in range(nz // per + 1):
        east = west = jnp.zeros(shape, jnp.float32)
        for i in range(per):
            k, start = j * per + i, i * nt
            if k > nz:
                break
            index = lax.rem(2 * (lane - start + cols), cols)
            if k == nz:
                side = (jnp.broadcast_to(kmt[:, cols - 1 :], shape), jnp.broadcast_to(kmt[:, :1], shape))
            else:
                side = pick(pairs[k], lax.rem(index + cols - 1, cols)), pick(pairs[k], index)
            east, west = (jnp.where(lane >= start, a, b) for a, b in zip(side, (east, west)))
        east_ref[pl.ds(j * rows, rows), :] = east
        west_ref[pl.ds(j * rows, rows), :] = west
    for t in range(nt):
        start = t * nz * rows
        put_rows(x_ref[pl.ds(start, nz, stride=rows), :], x_ref[pl.ds(start + rows - 1, nz, stride=rows), :], t * nz)
    put_rows(jnp.broadcast_to(kmt[:1], (nz, cols)), jnp.broadcast_to(kmt[rows - 1 :], (nz, cols)), nt * nz)


def starts_early():
    _, _, top = position()
    return (lax.axis_index("lon") == 0) & jnp.logical_not(top)


def early_kernel(dims, x_ref, kmt_ref, *refs):
    @pl.when(starts_early())
    def _():
        coefs_body(dims, x_ref, kmt_ref, *refs[4:])
        inner_body(dims, 0, EARLY, x_ref, kmt_ref, *refs)


def late_kernel(dims, x_ref, kmt_ref, *refs):
    refs = refs[len(refs) // 2 :]
    early = starts_early()

    @pl.when(jnp.logical_not(early))
    def _():
        coefs_body(dims, x_ref, kmt_ref, *refs[4:])

    inner_body(dims, jnp.where(early, EARLY, 0), dims[0] // UNROLL, x_ref, kmt_ref, *refs)


def coefs_body(dims, x_ref, kmt_ref, sum_x_ref, sum_y_ref, inner_ref, ax_ref, bx_ref, ay_ref, by_ref):
    _, nz, rows, cols, _ = dims
    shape = (rows, cols)
    lane, row = lanes_of(shape), rows_of(shape)
    kmt = kmt_ref[...]
    heat = [x_ref[pl.ds(k * rows, rows), :] for k in range(nz)]
    salt = [x_ref[pl.ds((nz + k) * rows, rows), :] for k in range(nz)]
    density = [density_of(h, s) for h, s in zip(heat, salt)]
    wm = [as_mask(kmt > k + 1) for k in range(nz - 1)]
    kmt_w = pltpu.roll(kmt, 1, 1)
    strat = [0.5 * s for s in level_lists(density, wm)[1]]
    kmt_x = jnp.where(lane == 0, 0.0, jnp.minimum(kmt, kmt_w))
    kmt_y = jnp.where(row == 0, 0.0, jnp.minimum(kmt, pltpu.roll(kmt, 1, 0)))
    for k in range(nz):
        part = pl.ds(k * rows, rows)
        mask = as_mask(kmt_x > k)
        slope = slope_at(density[k], pltpu.roll(density[k], 1, 1), mask, strat[k], pltpu.roll(strat[k], 1, 1))
        ax_ref[part, :] = REDI * mask
        bx_ref[part, :] = FACE * slope
        sum_x_ref[part, :] = slope + pltpu.roll(slope, cols - 1, 1)
        inner_ref[part, :] = pair_of(slope[:, 1:2], slope[:, cols - 1 :])
        mask = as_mask(kmt_y > k)
        slope = slope_at(density[k], pltpu.roll(density[k], 1, 0), mask, strat[k], pltpu.roll(strat[k], 1, 0))
        ay_ref[part, :] = REDI * mask
        by_ref[part, :] = FACE * slope
        sum_y_ref[part, :] = slope + pltpu.roll(slope, rows - 1, 0)


def inner_body(dims, first, last, x_ref, kmt_ref, base_ref, cx_ref, cy_ref, diff_ref, sum_x_ref, sum_y_ref, inner_ref,
               ax_ref, bx_ref, ay_ref, by_ref):
    _, nz, rows, cols, _ = dims
    kmt = kmt_ref[...]
    kmt_w = pltpu.roll(kmt, 1, 1)
    wm = [as_mask(kmt > k + 1) for k in range(nz - 1)]
    wm_w = [as_mask(kmt_w > k + 1) for k in range(nz - 1)]

    def load(ref, k):
        return ref[pl.ds(k * rows, rows), :]

    def tracer(t):
        base = t * (nz * rows)
        part = lambda k: pl.ds(pl.multiple_of(base + k * rows, rows), rows)
        value = [x_ref[part(k), :] for k in range(nz)]
        beside = [pltpu.roll(v, 1, 1) for v in value]
        diff, total = level_lists(value, wm)
        total_w = level_lists(beside, wm_w)[1]
        cell_x, cell_y = [], []
        for k in range(nz):
            grad = load(ax_ref, k) * (value[k] - beside[k])
            flux = grad + load(bx_ref, k) * (total[k] + total_w[k])
            cell_x.append(grad + pltpu.roll(grad, cols - 1, 1))
            gain = pltpu.roll(flux, cols - 1, 1) - flux
            grad = load(ay_ref, k) * (value[k] - pltpu.roll(value[k], 1, 0))
            flux = grad + load(by_ref, k) * (total[k] + pltpu.roll(total[k], 1, 0))
            cell_y.append(grad + pltpu.roll(grad, rows - 1, 0))
            base_ref[part(k), :] = value[k] + (gain + (pltpu.roll(flux, rows - 1, 0) - flux))
        for k in range(nz - 1):
            cx_ref[part(k), :] = cell_x[k] + cell_x[k + 1]
            cy_ref[part(k), :] = cell_y[k] + cell_y[k + 1]
            diff_ref[part(k), :] = diff[k]

    def block(i, carry):
        for t in range(UNROLL):
            tracer(i * UNROLL + t)
        return carry

    lax.fori_loop(first, last, block, 0)


def outer_kernel(dims, x_ref, kmt_ref, own_ref, base_ref, cx_ref, cy_ref, diff_ref, sum_x_ref, sum_y_ref, inner_ref,
                 from_west, from_east, even_ref, odd_ref, out_hbm, out_ref, p_ref, q_ref, z_ref, side_ref, sems):
    nt, nz, rows, cols, _ = dims
    per = cols // nt
    shape = (rows, cols)
    lane, row = lanes_of(shape), rows_of(shape)
    odd, bottom, _ = position()
    kmt = kmt_ref[...]

    def load(ref, k):
        return ref[pl.ds(k * rows, rows), :]

    even_lane = lax.rem(lane, 2) == 0
    slot = jnp.where(even_lane, lane // 2, lax.rem(lane + 1, cols) // 2)
    outward = jnp.where(even_lane, -1.0, 1.0)

    def ghost_at(k):
        index = lax.rem(slot + (k % per) * nt, cols)
        return jnp.where(even_lane, pick(load(from_west, k // per), index), pick(load(from_east, k // per), index))

    own = [load(own_ref, k) for k in range(nz)]
    ghost = [ghost_at(k) for k in range(nz + 1)]
    own_kmt, ghost_kmt = pair_of(kmt[:, :1], kmt[:, cols - 1 :]), ghost.pop()
    own_wm = [as_mask(own_kmt > k + 1) for k in range(nz - 1)]
    ghost_wm = [as_mask(ghost_kmt > k + 1) for k in range(nz - 1)]
    side_mask = [as_mask(jnp.minimum(own_kmt, ghost_kmt) > k) for k in range(nz)]

    def side_density(values):
        return [density_of(v, pltpu.roll(v, cols - 2, 1)) for v in values]

    own_density, ghost_density = side_density(own), side_density(ghost)
    own_strat = level_lists(own_density, own_wm)[1]
    ghost_strat = level_lists(ghost_density, ghost_wm)[1]
    first = [
        outward * slope_at(ghost_density[k], own_density[k], side_mask[k], 0.5 * own_strat[k], 0.5 * ghost_strat[k])
        for k in range(nz)
    ]
    side_slope = [pair_of(s[:, :1], s[:, cols - 1 :]) for s in first]
    outer = (lane == 0) | (lane == cols - 1)
    sum_x = [load(sum_x_ref, k) + jnp.where(outer, first[k], 0.0) for k in range(nz)]

    flat = (nz, cols)
    level = rows_of(flat).astype(jnp.float32)

    def ends(index):
        a, b = even_ref[pl.ds(index, nz), :], odd_ref[pl.ds(index, nz), :]
        return jnp.where(odd, a, b), jnp.where(odd, b, a)

    def own_rows(t):
        start = t * nz * rows
        return x_ref[pl.ds(start, nz, stride=rows), :], x_ref[pl.ds(start + rows - 1, nz, stride=rows), :]

    south_kmt, north_kmt = ends(nt * nz)
    south_kmt = jnp.where(bottom, 0.0, south_kmt)
    low_kmt, high_kmt = jnp.broadcast_to(kmt[:1], flat), jnp.broadcast_to(kmt[rows - 1 :], flat)

    def end_slope(kmts, heats, salts):
        masks = [as_mask(k > level + 1.0) for k in kmts]
        mask = as_mask(jnp.minimum(*kmts) > level)
        densities = [density_of(h, s) for h, s in zip(heats, salts)]
        strats = [0.5 * level_rows(d, m)[1] for d, m in zip(densities, masks)]
        return masks, mask, slope_at(densities[1], densities[0], mask, *strats)

    heat_ends, salt_ends, heat_own, salt_own = ends(0), ends(nz), own_rows(0), own_rows(1)
    south = end_slope((south_kmt, low_kmt), (heat_ends[0], heat_own[0]), (salt_ends[0], salt_own[0]))
    north = end_slope((high_kmt, north_kmt), (heat_own[1], heat_ends[1]), (salt_own[1], salt_ends[1]))
    sum_y = []
    for k in range(nz):
        below, above = jnp.broadcast_to(south[2][k : k + 1], shape), jnp.broadcast_to(north[2][k : k + 1], shape)
        sum_y.append(load(sum_y_ref, k) + jnp.where(row == 0, below, jnp.where(row == rows - 1, above, 0.0)))

    for k in range(nz - 1):
        part = pl.ds(k * rows, rows)
        wm = as_mask(kmt > k + 1)
        level_x, level_y = 0.25 * (sum_x[k] + sum_x[k + 1]), 0.25 * (sum_y[k] + sum_y[k + 1])
        p_ref[part, :] = LEVEL * level_x * wm
        q_ref[part, :] = LEVEL * level_y * wm
        z_ref[part, :] = REDI * (level_x * level_x + level_y * level_y) * wm
    q_ref[pl.ds((nz - 1) * rows, rows), :] = jnp.zeros(shape, jnp.float32)

    own_sum, ghost_sum = level_lists(own, own_wm)[1], level_lists(ghost, ghost_wm)[1]
    grad = [REDI * side_mask[k] * (ghost[k] - own[k]) for k in range(nz)]
    flux = [grad[k] + outward * FACE * side_slope[k] * (own_sum[k] + ghost_sum[k]) for k in range(nz)]
    both = [side_slope[k] + load(inner_ref, k) for k in range(nz)]
    tilt = [0.25 * LEVEL * (both[k] + both[k + 1]) * own_wm[k] * outward * (grad[k] + grad[k + 1]) for k in range(nz - 1)]
    for k in range(nz):
        added = flux[k]
        if k < nz - 1:
            added = added + tilt[k]
        if k > 0:
            added = added - tilt[k - 1]
        side_ref[pl.ds(k * rows, rows), :] = added

    end_coefs = []
    for (wms, mask, slope), start in ((south, 0), (north, rows - 1)):
        end_coefs.append((wms, REDI * mask, FACE * slope, q_ref[pl.ds(start, nz, stride=rows), :]))

    def cell_step(t):
        base = t * nz * rows
        part = lambda k: pl.ds(base + k * rows, rows)
        down = None
        for k in range(nz):
            side = load(side_ref, k)
            side = pltpu.roll(side, cols - 2 * t, 1) if t else side
            result = base_ref[part(k), :] + jnp.where(outer, side, 0.0)
            if k > 0:
                result = result - down
            if k < nz - 1:
                down = load(p_ref, k) * cx_ref[part(k), :] + load(q_ref, k) * cy_ref[part(k), :] + load(z_ref, k) * diff_ref[part(k), :]
                result = result + down
            out_ref[part(k), :] = result

    def end_step(t):
        for end in (0, 1):
            wms, a, b, q = end_coefs[end]
            here, there = own_rows(t)[end], ends(t * nz)[end]
            below, above = (there, here) if end == 0 else (here, there)
            sums = level_rows(below, wms[0])[1] + level_rows(above, wms[1])[1]
            grad = a * (above - below)
            flux = grad + b * sums
            tilt = q * (grad + pltpu.roll(grad, nz - 1, 0))
            gain = flux if end == 1 else -flux
            part = pl.ds(t * nz * rows + (rows - 1 if end else 0), nz, stride=rows)
            out_ref[part, :] = out_ref[part, :] + (gain + (tilt - pltpu.roll(tilt, 1, 0)))

    step = nt // CHUNKS
    copies = []
    for c in range(CHUNKS):
        for t in range(c * step, (c + 1) * step):
            cell_step(t)
        for t in range(c * step, (c + 1) * step):
            end_step(t)
        part = pl.ds(c * step * nz * rows, step * nz * rows)
        copies.append(pltpu.make_async_copy(out_ref.at[part], out_hbm.at[part], sems.at[c]))
        copies[-1].start()
    for copy in copies:
        copy.wait()


def row_pairs(color, lons, lats):
    pairs = []
    for lon in range(lons):
        for lat in range(lats - 1):
            if lat % 2 == color:
                pairs += [(lon * lats + lat, lon * lats + lat + 1), (lon * lats + lat + 1, lon * lats + lat)]
        if (lats - 1) % 2 == color:
            pairs.append((lon * lats + lats - 1, (lons - 1 - lon) * lats + lats - 1))
    free_in = sorted(set(range(lons * lats)) - {b for _, b in pairs})
    free_out = set(range(lons * lats)) - {a for a, _ in pairs}
    for target in free_in:
        lon, lat = divmod(target, lats)
        source = (lon ^ 1 if lons % 2 == 0 else (lon + 1) % lons) * lats + lat
        assert source in free_out
        pairs.append((source, target))
    return pairs


def local(tracers, kmt):
    nt, nz, rows, cols = tracers.shape
    lons, lats = lax.axis_size("lon"), lax.axis_size("lat")
    dims = (nt, nz, rows, cols, (lats - 1) % 2)
    packed = ((nz // (cols // nt) + 1) * rows, cols)
    edge = (nt * nz + nz, cols)
    level, block = (nz * rows, cols), (nt * nz * rows, cols)
    vmem, anywhere = pl.BlockSpec(memory_space=pltpu.VMEM), pl.BlockSpec(memory_space=pl.ANY)

    def call(kernel, inputs, out_shape, scratch, flops, specs=None, aliases={}):
        out = [pltpu.VMEM(s, jnp.float32) for s in out_shape] if specs is None else out_shape
        if specs is None:
            specs = [vmem] * len(out_shape)
        near = [pltpu.with_memory_space_constraint(a, pltpu.HBM if a is x or a is kmt else pltpu.VMEM) for a in inputs]
        return pl.pallas_call(
            functools.partial(kernel, dims),
            out_shape=out,
            in_specs=[anywhere if a is x or a is kmt else vmem for a in inputs],
            out_specs=specs,
            scratch_shapes=scratch,
            input_output_aliases=aliases,
            cost_estimate=pl.CostEstimate(flops=flops, bytes_accessed=flops, transcendentals=0),
            compiler_params=pltpu.CompilerParams(vmem_limit_bytes=16 * 2**20),
        )(*near)

    x = tracers.reshape(block)
    cells = lambda levels: pltpu.VMEM((levels * rows, cols), jnp.float32)
    near, own, east, west, even, odd, near_kmt = call(
        pack_kernel,
        (x, kmt),
        (block, level, packed, packed, edge, edge, (rows, cols)),
        [pltpu.VMEM((rows, cols), jnp.int32), pltpu.SemaphoreType.DMA((CHUNKS + 1,))],
        1000000,
    )
    ring = [(i, (i + 1) % lons) for i in range(lons)]
    from_west = lax.ppermute(east, "lon", ring)
    shapes = (block,) * 4 + (level,) * 7
    inner = call(early_kernel, (near, near_kmt), shapes, [], 10000000)
    from_odd = lax.ppermute(odd, ("lon", "lat"), row_pairs(1, lons, lats))
    from_even = lax.ppermute(even, ("lon", "lat"), row_pairs(0, lons, lats))
    from_east = lax.ppermute(west, "lon", [(b, a) for a, b in ring])
    aliases = {2 + i: i for i in range(len(shapes))}
    inner = call(late_kernel, (near, near_kmt, *inner), shapes, [], 10000000, aliases=aliases)[:7]
    out = call(
        outer_kernel,
        (near, near_kmt, own, *inner, from_west, from_east, from_even, from_odd),
        jax.ShapeDtypeStruct(block, jnp.float32),
        [pltpu.VMEM(block, jnp.float32), cells(nz - 1), cells(nz), cells(nz - 1), cells(nz), pltpu.SemaphoreType.DMA((CHUNKS,))],
        10000000,
        anywhere,
    )
    return out.reshape(tracers.shape)


def solution(mesh):
    return jax.shard_map(
        local,
        mesh=mesh,
        in_specs=(P(None, None, "lat", "lon"), P("lat", "lon")),
        out_specs=P(None, None, "lat", "lon"),
        check_vma=False,
    )
```

```python
import functools

import jax
import jax.numpy as jnp
from jax import lax
from jax.experimental import pallas as pl
from jax.experimental.pallas import tpu as pltpu
from jax.sharding import PartitionSpec as P

THERMAL = 0.2
HALINE = 0.8
REDI = 0.1
SKEW = 0.05
SLOPE_MAX = 0.6
SLOPE_WIDTH = 0.2
FACE = 0.25 * (REDI - SKEW)
LEVEL = 0.25 * (REDI + SKEW) / REDI
LOADS = (0.5, 1.0)
STORES = (0.2, 0.4, 0.6, 0.8, 1.0)
UNROLL = 4
EARLY = 5


def taper(slope):
    return slope * 0.5 * (1.0 + jnp.tanh((SLOPE_MAX - jnp.abs(slope)) * (1.0 / SLOPE_WIDTH)))


def lanes_of(shape):
    return lax.broadcasted_iota(jnp.int32, shape, len(shape) - 1)


def rows_of(shape):
    return lax.broadcasted_iota(jnp.int32, shape, len(shape) - 2)


def density_of(heat, salt):
    return HALINE * salt - THERMAL * heat


def as_mask(flag):
    return jnp.where(flag, 1.0, 0.0)


def slope_at(here, there, mask, strat_here, strat_there):
    return taper((here - there) * mask / jnp.maximum(0.5 * (strat_here + strat_there), 1.0))


def level_lists(values, masks):
    diffs = [(values[k + 1] - values[k]) * masks[k] for k in range(len(values) - 1)]
    sums = [diffs[0]] + [a + b for a, b in zip(diffs, diffs[1:])] + [diffs[-1]]
    return diffs, sums


def level_rows(values, mask):
    diffs = (pltpu.roll(values, values.shape[0] - 1, 0) - values) * mask
    return diffs, diffs + pltpu.roll(diffs, 1, 0)


def position():
    lat = lax.axis_index("lat")
    return lax.rem(lat, 2) == 1, lat == 0, lat == lax.axis_size("lat") - 1


def pick(values, index):
    return jnp.take_along_axis(values, index, axis=1, mode="promise_in_bounds")


def pair_of(west, east, cols=128):
    shape = (west.shape[0], cols)
    return jnp.where(lax.rem(lanes_of(shape), 2) == 0, jnp.broadcast_to(west, shape), jnp.broadcast_to(east, shape))


def pack_kernel(dims, x_hbm, kmt_hbm, x_ref, own_ref, east_ref, west_ref, kmt_ref, raw_ref, sems):
    nt, nz, rows, cols, _ = dims
    per = cols // nt
    bounds = chunk_bounds(nt, LOADS)
    kmt_copy = pltpu.make_async_copy(kmt_hbm, raw_ref, sems.at[len(bounds)])
    kmt_copy.start()
    copies = []
    for c, (first, last) in enumerate(bounds):
        part = pl.ds(first * nz * rows, (last - first) * nz * rows)
        copies.append(pltpu.make_async_copy(x_hbm.at[part], x_ref.at[part], sems.at[c]))
        copies[-1].start()
    shape = (rows, cols)
    lane = lanes_of(shape)
    pairs = [jnp.zeros(shape, jnp.float32)] * nz
    for c, (first, last) in enumerate(bounds):
        copies[c].wait()
        for t in range(first, last):
            here = (lane == 2 * t) | (lane == (2 * t - 1) % cols)
            for k in range(nz):
                value = x_ref[pl.ds((t * nz + k) * rows, rows), :]
                pairs[k] = jnp.where(here, pltpu.roll(value, 2 * t, 1) if t else value, pairs[k])
    kmt_copy.wait()
    kmt = raw_ref[...].astype(jnp.float32)
    kmt_ref[...] = kmt
    for k in range(nz):
        own_ref[pl.ds(k * rows, rows), :] = pairs[k]
    for j in range(nz // per + 1):
        east = west = jnp.zeros(shape, jnp.float32)
        for i in range(per):
            k, start = j * per + i, i * nt
            if k > nz:
                break
            index = lax.rem(2 * (lane - start + cols), cols)
            if k == nz:
                side = (jnp.broadcast_to(kmt[:, cols - 1 :], shape), jnp.broadcast_to(kmt[:, :1], shape))
            else:
                side = pick(pairs[k], lax.rem(index + cols - 1, cols)), pick(pairs[k], index)
            east, west = (jnp.where(lane >= start, a, b) for a, b in zip(side, (east, west)))
        east_ref[pl.ds(j * rows, rows), :] = east
        west_ref[pl.ds(j * rows, rows), :] = west


def chunk_bounds(nt, shares):
    ends = [round(nt * share) for share in shares]
    return list(zip([0] + ends, ends))


def pairs_of(west_ref, east_ref, dims, count):
    nt, _, rows, cols, _ = dims
    per = cols // nt
    lane = lanes_of((rows, cols))
    even = lax.rem(lane, 2) == 0
    slot = jnp.where(even, lane // 2, lax.rem(lane + 1, cols) // 2)
    pairs = []
    for k in range(count):
        index = lax.rem(slot + (k % per) * nt, cols)
        part = pl.ds((k // per) * rows, rows)
        pairs.append(jnp.where(even, pick(west_ref[part, :], index), pick(east_ref[part, :], index)))
    return pairs


def early_blocks():
    odd, _, top = position()
    first = lax.axis_index("lon") == 0
    return jnp.where(first & odd & jnp.logical_not(top), EARLY, 0), jnp.where(first & jnp.logical_not(odd), EARLY, 0)


def ends_body(dims, x_ref, kmt_ref, even_ref, odd_ref):
    nt, nz, rows, cols, mirror_color = dims
    odd, _, top = position()

    def put_rows(low, high, start):
        index = lanes_of(low.shape)
        turned = pick(high, jnp.where(top, cols - 1 - index, index))
        for color, ref in ((0, even_ref), (1, odd_ref)):
            up = turned if color == mirror_color else high
            goes_up = odd if color == 1 else jnp.logical_not(odd)
            ref[pl.ds(start, nz), :] = jnp.where(goes_up, up, low)

    kmt = kmt_ref[...]
    put_rows(jnp.broadcast_to(kmt[:1], (nz, cols)), jnp.broadcast_to(kmt[rows - 1 :], (nz, cols)), nt * nz)
    for t in range(nt):
        start = t * nz * rows
        put_rows(x_ref[pl.ds(start, nz, stride=rows), :], x_ref[pl.ds(start + rows - 1, nz, stride=rows), :], t * nz)


def early_kernel(dims, x_ref, kmt_ref, *refs):
    *refs, even_ref, odd_ref = refs
    ends_body(dims, x_ref, kmt_ref, even_ref, odd_ref)
    early, _ = early_blocks()

    @pl.when(early > 0)
    def _():
        coefs_body(dims, x_ref, kmt_ref, *refs[2:])
        inner_body(dims, 0, early, x_ref, kmt_ref, *refs)


def middle_kernel(dims, x_ref, kmt_ref, *refs):
    refs = refs[len(refs) // 2 :]
    _, middle = early_blocks()

    @pl.when(middle > 0)
    def _():
        coefs_body(dims, x_ref, kmt_ref, *refs[2:])
        inner_body(dims, 0, middle, x_ref, kmt_ref, *refs)


def late_kernel(dims, x_ref, kmt_ref, *refs):
    refs = refs[len(refs) // 2 :]
    early, middle = early_blocks()

    @pl.when(early + middle == 0)
    def _():
        coefs_body(dims, x_ref, kmt_ref, *refs[2:])

    inner_body(dims, early + middle, dims[0] // UNROLL, x_ref, kmt_ref, *refs)


def coefs_body(dims, x_ref, kmt_ref, sum_y_ref, inner_ref, dense_ref, cell_w_ref, cell_e_ref, ax_ref, bx_ref, ay_ref, by_ref, p_ref, pw_ref, q_ref, z_ref):
    _, nz, rows, cols, _ = dims
    shape = (rows, cols)
    lane, row = lanes_of(shape), rows_of(shape)
    kmt = kmt_ref[...]
    heat = [x_ref[pl.ds(k * rows, rows), :] for k in range(nz)]
    salt = [x_ref[pl.ds((nz + k) * rows, rows), :] for k in range(nz)]
    density = [density_of(h, s) for h, s in zip(heat, salt)]
    wm = [as_mask(kmt > k + 1) for k in range(nz - 1)]
    kmt_w = pltpu.roll(kmt, 1, 1)
    strat = [0.5 * s for s in level_lists(density, wm)[1]]
    kmt_x = jnp.where(lane == 0, 0.0, jnp.minimum(kmt, kmt_w))
    kmt_y = jnp.where(row == 0, 0.0, jnp.minimum(kmt, pltpu.roll(kmt, 1, 0)))
    sum_x, sum_y = [], []
    for k in range(nz):
        part = pl.ds(k * rows, rows)
        mask = as_mask(kmt_x > k)
        slope = slope_at(density[k], pltpu.roll(density[k], 1, 1), mask, strat[k], pltpu.roll(strat[k], 1, 1))
        ax_ref[part, :] = REDI * mask
        bx_ref[part, :] = FACE * slope
        sum_x.append(slope + pltpu.roll(slope, cols - 1, 1))
        inner_ref[part, :] = pair_of(slope[:, 1:2], slope[:, cols - 1 :])
        mask = as_mask(kmt_y > k)
        slope = slope_at(density[k], pltpu.roll(density[k], 1, 0), mask, strat[k], pltpu.roll(strat[k], 1, 0))
        ay_ref[part, :] = REDI * mask
        by_ref[part, :] = FACE * slope
        sum_y.append(slope + pltpu.roll(slope, rows - 1, 0))
        sum_y_ref[part, :] = sum_y[k]
        dense_ref[part, :] = pair_of(density[k][:, :1], density[k][:, cols - 1 :])
        cell_w_ref[part, :] = jnp.zeros(shape, jnp.float32)
        cell_e_ref[part, :] = jnp.zeros(shape, jnp.float32)
    for k in range(nz - 1):
        part = pl.ds(k * rows, rows)
        level_x, level_y = 0.25 * (sum_x[k] + sum_x[k + 1]), 0.25 * (sum_y[k] + sum_y[k + 1])
        p = LEVEL * level_x * wm[k]
        p_ref[part, :] = p
        pw_ref[part, :] = pltpu.roll(p, 1, 1)
        q_ref[part, :] = LEVEL * level_y * wm[k]
        z_ref[part, :] = REDI * (level_x * level_x + level_y * level_y) * wm[k]


def inner_body(dims, first, last, x_ref, kmt_ref, base_ref, cy_ref, sum_y_ref, inner_ref, dense_ref, cell_w_ref, cell_e_ref,
               ax_ref, bx_ref, ay_ref, by_ref, p_ref, pw_ref, q_ref, z_ref):
    _, nz, rows, cols, _ = dims
    lane = lanes_of((rows, cols))
    kmt = kmt_ref[...]
    kmt_w = pltpu.roll(kmt, 1, 1)
    wm = [as_mask(kmt > k + 1) for k in range(nz - 1)]
    wm_w = [as_mask(kmt_w > k + 1) for k in range(nz - 1)]

    def load(ref, k):
        return ref[pl.ds(k * rows, rows), :]

    def tracer(t):
        base = t * (nz * rows)
        part = lambda k: pl.ds(pl.multiple_of(base + k * rows, rows), rows)
        value = [x_ref[part(k), :] for k in range(nz)]
        beside = [pltpu.roll(v, 1, 1) for v in value]
        diff, total = level_lists(value, wm)
        total_w = level_lists(beside, wm_w)[1]
        at_east, at_west = lane == lax.rem(2 * t + cols - 1, cols), lane == 2 * t + 1
        new, grads, fluxes, cell_y = [], [], [], []
        for k in range(nz):
            grad = load(ax_ref, k) * (value[k] - beside[k])
            grads.append(grad)
            fluxes.append(grad + load(bx_ref, k) * (total[k] + total_w[k]))
            grad = load(ay_ref, k) * (value[k] - pltpu.roll(value[k], 1, 0))
            flux = grad + load(by_ref, k) * (total[k] + pltpu.roll(total[k], 1, 0))
            cell_y.append(grad + pltpu.roll(grad, rows - 1, 0))
            new.append((value[k] - fluxes[k]) + (pltpu.roll(flux, rows - 1, 0) - flux))
        down = down_w = None
        for k in range(nz):
            result, west = new[k], fluxes[k]
            if k > 0:
                result, west = result - down, west - down_w
            if k < nz - 1:
                both_x, both_y = grads[k] + grads[k + 1], cell_y[k] + cell_y[k + 1]
                down = load(p_ref, k) * both_x + load(q_ref, k) * both_y + load(z_ref, k) * diff[k]
                down_w = load(pw_ref, k) * both_x
                result, west = result + down, west + down_w
                cy_ref[part(k), :] = both_y
                moved = pltpu.roll(both_x, lax.rem(2 * t, cols), 1)
                cell_e_ref[pl.ds(k * rows, rows), :] = jnp.where(at_east, moved, load(cell_e_ref, k))
                cell_w_ref[pl.ds(k * rows, rows), :] = jnp.where(at_west, moved, load(cell_w_ref, k))
            else:
                cy_ref[part(k), :] = jnp.zeros((rows, cols), jnp.float32)
            base_ref[part(k), :] = result + pltpu.roll(west, cols - 1, 1)

    def block(i, carry):
        for t in range(UNROLL):
            tracer(i * UNROLL + t)
        return carry

    lax.fori_loop(first, last, block, 0)


def rows_kernel(dims, x_ref, kmt_ref, base_ref, cy_ref, sum_y_ref, even_ref, odd_ref, out_ref):
    nt, nz, rows, cols, _ = dims
    odd, bottom, _ = position()
    kmt = kmt_ref[...]
    flat = (nz, cols)
    level = rows_of(flat).astype(jnp.float32)

    def ends(index):
        a, b = even_ref[pl.ds(index, nz), :], odd_ref[pl.ds(index, nz), :]
        return jnp.where(odd, a, b), jnp.where(odd, b, a)

    def own_rows(ref, t):
        start = t * nz * rows
        return ref[pl.ds(start, nz, stride=rows), :], ref[pl.ds(start + rows - 1, nz, stride=rows), :]

    ghost_kmts = ends(nt * nz)
    ghost_kmts = jnp.where(bottom, 0.0, ghost_kmts[0]), ghost_kmts[1]
    own_kmts = jnp.broadcast_to(kmt[:1], flat), jnp.broadcast_to(kmt[rows - 1 :], flat)
    heats, salts = (own_rows(x_ref, 0), ends(0)), (own_rows(x_ref, 1), ends(nz))
    sums_before = own_rows(sum_y_ref, 0)
    end_coefs = []
    for end, sign in ((0, -1.0), (1, 1.0)):
        kmts = own_kmts[end], ghost_kmts[end]
        wms = [as_mask(k > level + 1.0) for k in kmts]
        mask = as_mask(jnp.minimum(*kmts) > level)
        densities = [density_of(h[end], s[end]) for h, s in zip(heats, salts)]
        strats = [0.5 * level_rows(d, m)[1] for d, m in zip(densities, wms)]
        slope = sign * slope_at(densities[1], densities[0], mask, *strats)
        before = 0.25 * (sums_before[end] + pltpu.roll(sums_before[end], nz - 1, 0))
        change = 0.25 * (slope + pltpu.roll(slope, nz - 1, 0))
        after = before + change
        own_wm = wms[0]
        end_coefs.append((wms, REDI * mask, sign * FACE * slope, sign * LEVEL * after * own_wm, LEVEL * change * own_wm,
                          REDI * change * (before + after) * own_wm))
    for t in range(nt):
        for end in (0, 1):
            wms, a, b, q, q_change, z_change = end_coefs[end]
            here, there = own_rows(x_ref, t)[end], ends(t * nz)[end]
            diff, own_sum = level_rows(here, wms[0])
            grad = a * (there - here)
            gain = grad + b * (own_sum + level_rows(there, wms[1])[1])
            tilt = q * (grad + pltpu.roll(grad, nz - 1, 0)) + q_change * own_rows(cy_ref, t)[end] + z_change * diff
            part = pl.ds(t * nz * rows + (rows - 1 if end else 0), nz, stride=rows)
            out_ref[part, :] = out_ref[part, :] + (gain + (tilt - pltpu.roll(tilt, 1, 0)))


def outer_kernel(dims, kmt_ref, own_ref, base_ref, inner_ref, dense_ref, cell_w_ref, cell_e_ref,
                 from_west, from_east, out_hbm, out_ref, side_ref, sems):
    nt, nz, rows, cols, _ = dims
    shape = (rows, cols)
    lane = lanes_of(shape)
    per = cols // nt
    even = lax.rem(lane, 2) == 0
    kmt = kmt_ref[...]

    def load(ref, k):
        return ref[pl.ds(k * rows, rows), :]

    def spread(k, t):
        start = (k % per) * nt + t
        return pair_of(load(from_west, k // per)[:, start : start + 1], load(from_east, k // per)[:, start : start + 1])

    outward = jnp.where(even, -1.0, 1.0)
    own = [load(own_ref, k) for k in range(nz)]
    ghost = pairs_of(from_west, from_east, dims, nz)
    own_kmt, ghost_kmt = pair_of(kmt[:, :1], kmt[:, cols - 1 :]), spread(nz, 0)
    own_density = [load(dense_ref, k) for k in range(nz)]
    ghost_density = [density_of(spread(k, 0), spread(k, 1)) for k in range(nz)]
    own_wm = [as_mask(own_kmt > k + 1) for k in range(nz - 1)]
    ghost_wm = [as_mask(ghost_kmt > k + 1) for k in range(nz - 1)]
    side_mask = [as_mask(jnp.minimum(own_kmt, ghost_kmt) > k) for k in range(nz)]
    own_strat = level_lists(own_density, own_wm)[1]
    ghost_strat = level_lists(ghost_density, ghost_wm)[1]
    side_slope = [
        outward * slope_at(ghost_density[k], own_density[k], side_mask[k], 0.5 * own_strat[k], 0.5 * ghost_strat[k])
        for k in range(nz)
    ]
    own_diff, own_sum = level_lists(own, own_wm)
    ghost_sum = level_lists(ghost, ghost_wm)[1]
    grad = [REDI * side_mask[k] * (ghost[k] - own[k]) for k in range(nz)]
    flux = [grad[k] + outward * FACE * side_slope[k] * (own_sum[k] + ghost_sum[k]) for k in range(nz)]
    tilt = []
    for k in range(nz - 1):
        before = 0.25 * (load(inner_ref, k) + load(inner_ref, k + 1))
        change = 0.25 * (side_slope[k] + side_slope[k + 1])
        after = before + change
        inner = jnp.where(even, pltpu.roll(load(cell_w_ref, k), cols - 1, 1), load(cell_e_ref, k))
        across = after * outward * (grad[k] + grad[k + 1]) + change * inner
        along = change * (before + after) * own_diff[k]
        tilt.append(own_wm[k] * (LEVEL * across + REDI * along))
    for k in range(nz):
        added = flux[k]
        if k < nz - 1:
            added = added + tilt[k]
        if k > 0:
            added = added - tilt[k - 1]
        side_ref[pl.ds(k * rows, rows), :] = added
    outer = (lane == 0) | (lane == cols - 1)
    copies = []
    for c, (first, last) in enumerate(chunk_bounds(nt, STORES)):
        for t in range(first, last):
            for k in range(nz):
                part = pl.ds((t * nz + k) * rows, rows)
                side = load(side_ref, k)
                side = pltpu.roll(side, cols - 2 * t, 1) if t else side
                out_ref[part, :] = base_ref[part, :] + jnp.where(outer, side, 0.0)
        part = pl.ds(first * nz * rows, (last - first) * nz * rows)
        copies.append(pltpu.make_async_copy(out_ref.at[part], out_hbm.at[part], sems.at[c]))
        copies[-1].start()
    for copy in copies:
        copy.wait()


def row_pairs(color, lons, lats):
    pairs = []
    for lon in range(lons):
        for lat in range(lats - 1):
            if lat % 2 == color:
                pairs += [(lon * lats + lat, lon * lats + lat + 1), (lon * lats + lat + 1, lon * lats + lat)]
        if (lats - 1) % 2 == color:
            pairs.append((lon * lats + lats - 1, (lons - 1 - lon) * lats + lats - 1))
    free_in = sorted(set(range(lons * lats)) - {b for _, b in pairs})
    free_out = set(range(lons * lats)) - {a for a, _ in pairs}
    for target in free_in:
        lon, lat = divmod(target, lats)
        source = (lon ^ 1 if lons % 2 == 0 else (lon + 1) % lons) * lats + lat
        assert source in free_out
        pairs.append((source, target))
    return pairs


def local(tracers, kmt):
    nt, nz, rows, cols = tracers.shape
    lons, lats = lax.axis_size("lon"), lax.axis_size("lat")
    dims = (nt, nz, rows, cols, (lats - 1) % 2)
    packed = ((nz // (cols // nt) + 1) * rows, cols)
    edge = (nt * nz + nz, cols)
    level, block = (nz * rows, cols), (nt * nz * rows, cols)
    vmem, anywhere = pl.BlockSpec(memory_space=pltpu.VMEM), pl.BlockSpec(memory_space=pl.ANY)

    def call(kernel, inputs, out_shape, scratch, flops, specs=None, aliases={}):
        out = [pltpu.VMEM(s, jnp.float32) for s in out_shape] if specs is None else out_shape
        if specs is None:
            specs = [vmem] * len(out_shape)
        near = [pltpu.with_memory_space_constraint(a, pltpu.HBM if a is x or a is kmt else pltpu.VMEM) for a in inputs]
        return pl.pallas_call(
            functools.partial(kernel, dims),
            out_shape=out,
            in_specs=[anywhere if a is x or a is kmt else vmem for a in inputs],
            out_specs=specs,
            scratch_shapes=scratch,
            input_output_aliases=aliases,
            cost_estimate=pl.CostEstimate(flops=flops, bytes_accessed=flops, transcendentals=0),
            compiler_params=pltpu.CompilerParams(vmem_limit_bytes=16 * 2**20),
        )(*near)

    x = tracers.reshape(block)
    near, own, east, west, near_kmt = call(
        pack_kernel,
        (x, kmt),
        (block, level, packed, packed, (rows, cols)),
        [pltpu.VMEM((rows, cols), jnp.int32), pltpu.SemaphoreType.DMA((len(LOADS) + 1,))],
        1000000,
    )
    ring = [(i, (i + 1) % lons) for i in range(lons)]
    from_west = lax.ppermute(east, "lon", ring)
    shapes = (block,) * 2 + (level,) * 13
    *inner, even, odd = call(early_kernel, (near, near_kmt), (*shapes, edge, edge), [], 10000000)
    from_odd = lax.ppermute(odd, ("lon", "lat"), row_pairs(1, lons, lats))
    aliases = {2 + i: i for i in range(len(shapes))}
    inner = call(middle_kernel, (near, near_kmt, *inner), shapes, [], 10000000, aliases=aliases)
    from_even = lax.ppermute(even, ("lon", "lat"), row_pairs(0, lons, lats))
    from_east = lax.ppermute(west, "lon", [(b, a) for a, b in ring])
    inner = call(late_kernel, (near, near_kmt, *inner), shapes, [], 10000000, aliases=aliases)
    base, cy, sum_y, inner_slope, dense, cell_w, cell_e = inner[:7]
    ends = (near, near_kmt, base, cy, sum_y, from_even, from_odd)
    (base,) = call(rows_kernel, ends, (block,), [], 1000000, aliases={2: 0})
    out = call(
        outer_kernel,
        (near_kmt, own, base, inner_slope, dense, cell_w, cell_e, from_west, from_east),
        jax.ShapeDtypeStruct(block, jnp.float32),
        [pltpu.VMEM(block, jnp.float32), pltpu.VMEM(level, jnp.float32), pltpu.SemaphoreType.DMA((len(STORES),))],
        10000000,
        anywhere,
    )
    return out.reshape(tracers.shape)


def solution(mesh):
    return jax.shard_map(
        local,
        mesh=mesh,
        in_specs=(P(None, None, "lat", "lon"), P("lat", "lon")),
        out_specs=P(None, None, "lat", "lon"),
        check_vma=False,
    )
```

```python
import functools

import jax
import jax.numpy as jnp
from jax import lax
from jax.experimental import pallas as pl
from jax.experimental.pallas import tpu as pltpu
from jax.sharding import PartitionSpec as P

THERMAL = 0.2
HALINE = 0.8
REDI = 0.1
SKEW = 0.05
SLOPE_MAX = 0.6
SLOPE_WIDTH = 0.2
FACE = 0.25 * (REDI - SKEW)
LEVEL = 0.25 * (REDI + SKEW) / REDI
LOADS = (0.5, 1.0)
STORES = (0.2, 0.4, 0.6, 0.8, 1.0)
UNROLL = 4
EVEN = (2, 6)
ODD = (5, 5)


def taper(slope):
    return slope * 0.5 * (1.0 + jnp.tanh((SLOPE_MAX - jnp.abs(slope)) * (1.0 / SLOPE_WIDTH)))


def lanes_of(shape):
    return lax.broadcasted_iota(jnp.int32, shape, len(shape) - 1)


def rows_of(shape):
    return lax.broadcasted_iota(jnp.int32, shape, len(shape) - 2)


def density_of(heat, salt):
    return HALINE * salt - THERMAL * heat


def as_mask(flag):
    return jnp.where(flag, 1.0, 0.0)


def slope_at(here, there, mask, strat_here, strat_there):
    return taper((here - there) * mask / jnp.maximum(0.5 * (strat_here + strat_there), 1.0))


def level_lists(values, masks):
    diffs = [(values[k + 1] - values[k]) * masks[k] for k in range(len(values) - 1)]
    sums = [diffs[0]] + [a + b for a, b in zip(diffs, diffs[1:])] + [diffs[-1]]
    return diffs, sums


def level_rows(values, mask):
    diffs = (pltpu.roll(values, values.shape[0] - 1, 0) - values) * mask
    return diffs, diffs + pltpu.roll(diffs, 1, 0)


def position():
    lat = lax.axis_index("lat")
    return lax.rem(lat, 2) == 1, lat == 0, lat == lax.axis_size("lat") - 1


def pick(values, index):
    return jnp.take_along_axis(values, index, axis=1, mode="promise_in_bounds")


def pair_of(west, east, cols=128):
    shape = (west.shape[0], cols)
    return jnp.where(lax.rem(lanes_of(shape), 2) == 0, jnp.broadcast_to(west, shape), jnp.broadcast_to(east, shape))


def pack_kernel(dims, x_hbm, kmt_hbm, x_ref, own_ref, east_ref, west_ref, kmt_ref, even_ref, odd_ref, raw_ref, sems):
    nt, nz, rows, cols, mirror_color = dims
    per = cols // nt
    bounds = chunk_bounds(nt, LOADS)
    kmt_copy = pltpu.make_async_copy(kmt_hbm, raw_ref, sems.at[len(bounds)])
    kmt_copy.start()
    copies = []
    for c, (first, last) in enumerate(bounds):
        part = pl.ds(first * nz * rows, (last - first) * nz * rows)
        copies.append(pltpu.make_async_copy(x_hbm.at[part], x_ref.at[part], sems.at[c]))
        copies[-1].start()
    shape = (rows, cols)
    lane = lanes_of(shape)
    odd, _, top = position()

    def put_rows(low, high, start):
        index = lanes_of(low.shape)
        turned = pick(high, jnp.where(top, cols - 1 - index, index))
        for color, ref in ((0, even_ref), (1, odd_ref)):
            up = turned if color == mirror_color else high
            goes_up = odd if color == 1 else jnp.logical_not(odd)
            ref[pl.ds(start, nz), :] = jnp.where(goes_up, up, low)

    pairs = [jnp.zeros(shape, jnp.float32)] * nz
    for c, (first, last) in enumerate(bounds):
        copies[c].wait()
        for t in range(first, last):
            here = (lane == 2 * t) | (lane == (2 * t - 1) % cols)
            for k in range(nz):
                value = x_ref[pl.ds((t * nz + k) * rows, rows), :]
                pairs[k] = jnp.where(here, pltpu.roll(value, 2 * t, 1) if t else value, pairs[k])
        for t in range(first, last):
            start = t * nz * rows
            put_rows(x_ref[pl.ds(start, nz, stride=rows), :], x_ref[pl.ds(start + rows - 1, nz, stride=rows), :], t * nz)
    kmt_copy.wait()
    kmt = raw_ref[...].astype(jnp.float32)
    kmt_ref[...] = kmt
    put_rows(jnp.broadcast_to(kmt[:1], (nz, cols)), jnp.broadcast_to(kmt[rows - 1 :], (nz, cols)), nt * nz)
    for k in range(nz):
        own_ref[pl.ds(k * rows, rows), :] = pairs[k]
    for j in range(nz // per + 1):
        east = west = jnp.zeros(shape, jnp.float32)
        for i in range(per):
            k, start = j * per + i, i * nt
            if k > nz:
                break
            index = lax.rem(2 * (lane - start + cols), cols)
            if k == nz:
                side = (jnp.broadcast_to(kmt[:, cols - 1 :], shape), jnp.broadcast_to(kmt[:, :1], shape))
            else:
                side = pick(pairs[k], lax.rem(index + cols - 1, cols)), pick(pairs[k], index)
            east, west = (jnp.where(lane >= start, a, b) for a, b in zip(side, (east, west)))
        east_ref[pl.ds(j * rows, rows), :] = east
        west_ref[pl.ds(j * rows, rows), :] = west


def chunk_bounds(nt, shares):
    ends = [round(nt * share) for share in shares]
    return list(zip([0] + ends, ends))


def pairs_of(west_ref, east_ref, dims, count):
    nt, _, rows, cols, _ = dims
    per = cols // nt
    lane = lanes_of((rows, cols))
    even = lax.rem(lane, 2) == 0
    slot = jnp.where(even, lane // 2, lax.rem(lane + 1, cols) // 2)
    pairs = []
    for k in range(count):
        index = lax.rem(slot + (k % per) * nt, cols)
        part = pl.ds((k // per) * rows, rows)
        pairs.append(jnp.where(even, pick(west_ref[part, :], index), pick(east_ref[part, :], index)))
    return pairs


def early_blocks():
    odd, _, top = position()
    first = (lax.axis_index("lon") == 0) & jnp.logical_not(top)
    return tuple(jnp.where(first, jnp.where(odd, b, a), 0) for a, b in zip(EVEN, ODD))


def early_kernel(dims, x_ref, kmt_ref, *refs):
    *refs, turned_ref = refs
    early, _ = early_blocks()

    @pl.when(early > 0)
    def _():
        coefs_body(dims, x_ref, kmt_ref, *refs[2:])
        inner_body(dims, 0, early, turned_ref, x_ref, kmt_ref, *refs)


def middle_kernel(dims, x_ref, kmt_ref, *refs):
    *refs, turned_ref = refs
    refs = refs[len(refs) // 2 :]
    inner_body(dims, *early_blocks(), turned_ref, x_ref, kmt_ref, *refs)


def late_kernel(dims, x_ref, kmt_ref, *refs):
    *refs, turned_ref = refs
    refs = refs[len(refs) // 2 :]
    _, done = early_blocks()

    @pl.when(done == 0)
    def _():
        coefs_body(dims, x_ref, kmt_ref, *refs[2:])

    inner_body(dims, done, dims[0] // UNROLL, turned_ref, x_ref, kmt_ref, *refs)


def coefs_body(dims, x_ref, kmt_ref, sum_y_ref, inner_ref, dense_ref, cell_w_ref, cell_e_ref, ax_ref, bx_ref, ay_ref, by_ref, p_ref, pw_ref, q_ref, z_ref):
    _, nz, rows, cols, _ = dims
    shape = (rows, cols)
    lane, row = lanes_of(shape), rows_of(shape)
    kmt = kmt_ref[...]
    heat = [x_ref[pl.ds(k * rows, rows), :] for k in range(nz)]
    salt = [x_ref[pl.ds((nz + k) * rows, rows), :] for k in range(nz)]
    density = [density_of(h, s) for h, s in zip(heat, salt)]
    wm = [as_mask(kmt > k + 1) for k in range(nz - 1)]
    kmt_w = pltpu.roll(kmt, 1, 1)
    strat = [0.5 * s for s in level_lists(density, wm)[1]]
    kmt_x = jnp.where(lane == 0, 0.0, jnp.minimum(kmt, kmt_w))
    kmt_y = jnp.where(row == 0, 0.0, jnp.minimum(kmt, pltpu.roll(kmt, 1, 0)))
    sum_x, sum_y = [], []
    for k in range(nz):
        part = pl.ds(k * rows, rows)
        mask = as_mask(kmt_x > k)
        slope = slope_at(density[k], pltpu.roll(density[k], 1, 1), mask, strat[k], pltpu.roll(strat[k], 1, 1))
        ax_ref[part, :] = REDI * mask
        bx_ref[part, :] = FACE * slope
        sum_x.append(slope + pltpu.roll(slope, cols - 1, 1))
        inner_ref[part, :] = pair_of(slope[:, 1:2], slope[:, cols - 1 :])
        mask = as_mask(kmt_y > k)
        slope = slope_at(density[k], pltpu.roll(density[k], 1, 0), mask, strat[k], pltpu.roll(strat[k], 1, 0))
        ay_ref[part, :] = REDI * mask
        by_ref[part, :] = FACE * slope
        sum_y.append(slope + pltpu.roll(slope, rows - 1, 0))
        sum_y_ref[part, :] = sum_y[k]
        dense_ref[part, :] = pair_of(density[k][:, :1], density[k][:, cols - 1 :])
        cell_w_ref[part, :] = jnp.zeros(shape, jnp.float32)
        cell_e_ref[part, :] = jnp.zeros(shape, jnp.float32)
    for k in range(nz - 1):
        part = pl.ds(k * rows, rows)
        level_x, level_y = 0.25 * (sum_x[k] + sum_x[k + 1]), 0.25 * (sum_y[k] + sum_y[k + 1])
        p = LEVEL * level_x * wm[k]
        p_ref[part, :] = p
        pw_ref[part, :] = pltpu.roll(p, 1, 1)
        q_ref[part, :] = LEVEL * level_y * wm[k]
        z_ref[part, :] = REDI * (level_x * level_x + level_y * level_y) * wm[k]


def inner_body(dims, first, last, turned_ref, x_ref, kmt_ref, base_ref, cy_ref, sum_y_ref, inner_ref, dense_ref, cell_w_ref, cell_e_ref,
               ax_ref, bx_ref, ay_ref, by_ref, p_ref, pw_ref, q_ref, z_ref):
    nt, nz, rows, cols, _ = dims
    lane = lanes_of((rows, cols))

    def load(ref, k):
        return ref[pl.ds(k * rows, rows), :]

    def turn(i):
        for j in range(UNROLL * nz):
            part = pl.ds(pl.multiple_of((i * UNROLL * nz + j) * rows, rows), rows)
            turned_ref[lax.rem(i, 2), pl.ds(j * rows, rows), :] = pltpu.roll(x_ref[part, :], 1, 1)

    def tracer(i, j, wm, wm_w):
        t = i * UNROLL + j
        base = t * (nz * rows)
        part = lambda k: pl.ds(pl.multiple_of(base + k * rows, rows), rows)
        value = [x_ref[part(k), :] for k in range(nz)]
        beside = [turned_ref[lax.rem(i, 2), pl.ds((j * nz + k) * rows, rows), :] for k in range(nz)]
        diff, total = level_lists(value, wm)
        total_w = level_lists(beside, wm_w)[1]
        at_east, at_west = lane == lax.rem(2 * t + cols - 1, cols), lane == 2 * t + 1
        new, grads, fluxes, cell_y = [], [], [], []
        for k in range(nz):
            grad = load(ax_ref, k) * (value[k] - beside[k])
            grads.append(grad)
            fluxes.append(grad + load(bx_ref, k) * (total[k] + total_w[k]))
            grad = load(ay_ref, k) * (value[k] - pltpu.roll(value[k], 1, 0))
            flux = grad + load(by_ref, k) * (total[k] + pltpu.roll(total[k], 1, 0))
            cell_y.append(grad + pltpu.roll(grad, rows - 1, 0))
            new.append((value[k] - fluxes[k]) + (pltpu.roll(flux, rows - 1, 0) - flux))
        down = down_w = None
        for k in range(nz):
            result, west = new[k], fluxes[k]
            if k > 0:
                result, west = result - down, west - down_w
            if k < nz - 1:
                both_x, both_y = grads[k] + grads[k + 1], cell_y[k] + cell_y[k + 1]
                down = load(p_ref, k) * both_x + load(q_ref, k) * both_y + load(z_ref, k) * diff[k]
                down_w = load(pw_ref, k) * both_x
                result, west = result + down, west + down_w
                cy_ref[part(k), :] = both_y
                moved = pltpu.roll(both_x, lax.rem(2 * t, cols), 1)
                cell_e_ref[pl.ds(k * rows, rows), :] = jnp.where(at_east, moved, load(cell_e_ref, k))
                cell_w_ref[pl.ds(k * rows, rows), :] = jnp.where(at_west, moved, load(cell_w_ref, k))
            else:
                cy_ref[part(k), :] = jnp.zeros((rows, cols), jnp.float32)
            base_ref[part(k), :] = result + pltpu.roll(west, cols - 1, 1)

    @pl.when(first < last)
    def _():
        kmt = kmt_ref[...]
        kmt_w = pltpu.roll(kmt, 1, 1)
        wm = [as_mask(kmt > k + 1) for k in range(nz - 1)]
        wm_w = [as_mask(kmt_w > k + 1) for k in range(nz - 1)]
        turn(first)

        def step(i, carry):
            for j in range(UNROLL):
                tracer(i, j, wm, wm_w)
            turn(jnp.minimum(i + 1, nt // UNROLL - 1))
            return carry

        lax.fori_loop(first, last, step, 0)


def rows_kernel(dims, x_ref, kmt_ref, base_ref, cy_ref, sum_y_ref, even_ref, odd_ref, out_ref):
    nt, nz, rows, cols, _ = dims
    odd, bottom, _ = position()
    kmt = kmt_ref[...]
    flat = (nz, cols)
    level = rows_of(flat).astype(jnp.float32)

    def ends(index):
        a, b = even_ref[pl.ds(index, nz), :], odd_ref[pl.ds(index, nz), :]
        return jnp.where(odd, a, b), jnp.where(odd, b, a)

    def own_rows(ref, t):
        start = t * nz * rows
        return ref[pl.ds(start, nz, stride=rows), :], ref[pl.ds(start + rows - 1, nz, stride=rows), :]

    ghost_kmts = ends(nt * nz)
    ghost_kmts = jnp.where(bottom, 0.0, ghost_kmts[0]), ghost_kmts[1]
    own_kmts = jnp.broadcast_to(kmt[:1], flat), jnp.broadcast_to(kmt[rows - 1 :], flat)
    heats, salts = (own_rows(x_ref, 0), ends(0)), (own_rows(x_ref, 1), ends(nz))
    sums_before = own_rows(sum_y_ref, 0)
    end_coefs = []
    for end, sign in ((0, -1.0), (1, 1.0)):
        kmts = own_kmts[end], ghost_kmts[end]
        wms = [as_mask(k > level + 1.0) for k in kmts]
        mask = as_mask(jnp.minimum(*kmts) > level)
        densities = [density_of(h[end], s[end]) for h, s in zip(heats, salts)]
        strats = [0.5 * level_rows(d, m)[1] for d, m in zip(densities, wms)]
        slope = sign * slope_at(densities[1], densities[0], mask, *strats)
        before = 0.25 * (sums_before[end] + pltpu.roll(sums_before[end], nz - 1, 0))
        change = 0.25 * (slope + pltpu.roll(slope, nz - 1, 0))
        after = before + change
        own_wm = wms[0]
        end_coefs.append((wms, REDI * mask, sign * FACE * slope, sign * LEVEL * after * own_wm, LEVEL * change * own_wm,
                          REDI * change * (before + after) * own_wm))
    for t in range(nt):
        for end in (0, 1):
            wms, a, b, q, q_change, z_change = end_coefs[end]
            here, there = own_rows(x_ref, t)[end], ends(t * nz)[end]
            diff, own_sum = level_rows(here, wms[0])
            grad = a * (there - here)
            gain = grad + b * (own_sum + level_rows(there, wms[1])[1])
            tilt = q * (grad + pltpu.roll(grad, nz - 1, 0)) + q_change * own_rows(cy_ref, t)[end] + z_change * diff
            part = pl.ds(t * nz * rows + (rows - 1 if end else 0), nz, stride=rows)
            out_ref[part, :] = out_ref[part, :] + (gain + (tilt - pltpu.roll(tilt, 1, 0)))


def outer_kernel(dims, kmt_ref, own_ref, base_ref, inner_ref, dense_ref, cell_w_ref, cell_e_ref,
                 from_west, from_east, out_hbm, out_ref, side_ref, sems):
    nt, nz, rows, cols, _ = dims
    shape = (rows, cols)
    lane = lanes_of(shape)
    per = cols // nt
    even = lax.rem(lane, 2) == 0
    kmt = kmt_ref[...]

    def load(ref, k):
        return ref[pl.ds(k * rows, rows), :]

    def spread(k, t):
        start = (k % per) * nt + t
        return pair_of(load(from_west, k // per)[:, start : start + 1], load(from_east, k // per)[:, start : start + 1])

    outward = jnp.where(even, -1.0, 1.0)
    own = [load(own_ref, k) for k in range(nz)]
    ghost = pairs_of(from_west, from_east, dims, nz)
    own_kmt, ghost_kmt = pair_of(kmt[:, :1], kmt[:, cols - 1 :]), spread(nz, 0)
    own_density = [load(dense_ref, k) for k in range(nz)]
    ghost_density = [density_of(spread(k, 0), spread(k, 1)) for k in range(nz)]
    own_wm = [as_mask(own_kmt > k + 1) for k in range(nz - 1)]
    ghost_wm = [as_mask(ghost_kmt > k + 1) for k in range(nz - 1)]
    side_mask = [as_mask(jnp.minimum(own_kmt, ghost_kmt) > k) for k in range(nz)]
    own_strat = level_lists(own_density, own_wm)[1]
    ghost_strat = level_lists(ghost_density, ghost_wm)[1]
    side_slope = [
        outward * slope_at(ghost_density[k], own_density[k], side_mask[k], 0.5 * own_strat[k], 0.5 * ghost_strat[k])
        for k in range(nz)
    ]
    own_diff, own_sum = level_lists(own, own_wm)
    ghost_sum = level_lists(ghost, ghost_wm)[1]
    grad = [REDI * side_mask[k] * (ghost[k] - own[k]) for k in range(nz)]
    flux = [grad[k] + outward * FACE * side_slope[k] * (own_sum[k] + ghost_sum[k]) for k in range(nz)]
    tilt = []
    for k in range(nz - 1):
        before = 0.25 * (load(inner_ref, k) + load(inner_ref, k + 1))
        change = 0.25 * (side_slope[k] + side_slope[k + 1])
        after = before + change
        inner = jnp.where(even, pltpu.roll(load(cell_w_ref, k), cols - 1, 1), load(cell_e_ref, k))
        across = after * outward * (grad[k] + grad[k + 1]) + change * inner
        along = change * (before + after) * own_diff[k]
        tilt.append(own_wm[k] * (LEVEL * across + REDI * along))
    for k in range(nz):
        added = flux[k]
        if k < nz - 1:
            added = added + tilt[k]
        if k > 0:
            added = added - tilt[k - 1]
        side_ref[pl.ds(k * rows, rows), :] = added
    outer = (lane == 0) | (lane == cols - 1)
    copies = []
    for c, (first, last) in enumerate(chunk_bounds(nt, STORES)):
        for t in range(first, last):
            for k in range(nz):
                part = pl.ds((t * nz + k) * rows, rows)
                side = load(side_ref, k)
                side = pltpu.roll(side, cols - 2 * t, 1) if t else side
                out_ref[part, :] = base_ref[part, :] + jnp.where(outer, side, 0.0)
        part = pl.ds(first * nz * rows, (last - first) * nz * rows)
        copies.append(pltpu.make_async_copy(out_ref.at[part], out_hbm.at[part], sems.at[c]))
        copies[-1].start()
    for copy in copies:
        copy.wait()


def row_pairs(color, lons, lats):
    pairs = []
    for lon in range(lons):
        for lat in range(lats - 1):
            if lat % 2 == color:
                pairs += [(lon * lats + lat, lon * lats + lat + 1), (lon * lats + lat + 1, lon * lats + lat)]
        if (lats - 1) % 2 == color:
            pairs.append((lon * lats + lats - 1, (lons - 1 - lon) * lats + lats - 1))
    free_in = sorted(set(range(lons * lats)) - {b for _, b in pairs})
    free_out = set(range(lons * lats)) - {a for a, _ in pairs}
    for target in free_in:
        lon, lat = divmod(target, lats)
        source = (lon ^ 1 if lons % 2 == 0 else (lon + 1) % lons) * lats + lat
        assert source in free_out
        pairs.append((source, target))
    return pairs


def local(tracers, kmt):
    nt, nz, rows, cols = tracers.shape
    lons, lats = lax.axis_size("lon"), lax.axis_size("lat")
    dims = (nt, nz, rows, cols, (lats - 1) % 2)
    packed = ((nz // (cols // nt) + 1) * rows, cols)
    edge = (nt * nz + nz, cols)
    level, block = (nz * rows, cols), (nt * nz * rows, cols)
    vmem, anywhere = pl.BlockSpec(memory_space=pltpu.VMEM), pl.BlockSpec(memory_space=pl.ANY)

    def call(kernel, inputs, out_shape, scratch, flops, specs=None, aliases={}):
        out = [pltpu.VMEM(s, jnp.float32) for s in out_shape] if specs is None else out_shape
        if specs is None:
            specs = [vmem] * len(out_shape)
        near = [pltpu.with_memory_space_constraint(a, pltpu.HBM if a is x or a is kmt else pltpu.VMEM) for a in inputs]
        return pl.pallas_call(
            functools.partial(kernel, dims),
            out_shape=out,
            in_specs=[anywhere if a is x or a is kmt else vmem for a in inputs],
            out_specs=specs,
            scratch_shapes=scratch,
            input_output_aliases=aliases,
            cost_estimate=pl.CostEstimate(flops=flops, bytes_accessed=flops, transcendentals=0),
            compiler_params=pltpu.CompilerParams(vmem_limit_bytes=16 * 2**20),
        )(*near)

    x = tracers.reshape(block)
    near, own, east, west, near_kmt, even, odd = call(
        pack_kernel,
        (x, kmt),
        (block, level, packed, packed, (rows, cols), edge, edge),
        [pltpu.VMEM((rows, cols), jnp.int32), pltpu.SemaphoreType.DMA((len(LOADS) + 1,))],
        1000000,
    )
    ring = [(i, (i + 1) % lons) for i in range(lons)]
    from_west = lax.ppermute(east, "lon", ring)
    shapes = (block,) * 2 + (level,) * 13
    turned = [pltpu.VMEM((2, UNROLL * nz * rows, cols), jnp.float32)]
    inner = call(early_kernel, (near, near_kmt), shapes, turned, 10000000)
    from_odd = lax.ppermute(odd, ("lon", "lat"), row_pairs(1, lons, lats))
    aliases = {2 + i: i for i in range(len(shapes))}
    inner = call(middle_kernel, (near, near_kmt, *inner), shapes, turned, 10000000, aliases=aliases)
    from_even = lax.ppermute(even, ("lon", "lat"), row_pairs(0, lons, lats))
    from_east = lax.ppermute(west, "lon", [(b, a) for a, b in ring])
    inner = call(late_kernel, (near, near_kmt, *inner), shapes, turned, 10000000, aliases=aliases)
    base, cy, sum_y, inner_slope, dense, cell_w, cell_e = inner[:7]
    ends = (near, near_kmt, base, cy, sum_y, from_even, from_odd)
    (base,) = call(rows_kernel, ends, (block,), [], 1000000, aliases={2: 0})
    out = call(
        outer_kernel,
        (near_kmt, own, base, inner_slope, dense, cell_w, cell_e, from_west, from_east),
        jax.ShapeDtypeStruct(block, jnp.float32),
        [pltpu.VMEM(block, jnp.float32), pltpu.VMEM(level, jnp.float32), pltpu.SemaphoreType.DMA((len(STORES),))],
        10000000,
        anywhere,
    )
    return out.reshape(tracers.shape)


def solution(mesh):
    return jax.shard_map(
        local,
        mesh=mesh,
        in_specs=(P(None, None, "lat", "lon"), P("lat", "lon")),
        out_specs=P(None, None, "lat", "lon"),
        check_vma=False,
    )
```

```python
import functools

import jax
import jax.numpy as jnp
from jax import lax
from jax.experimental import pallas as pl
from jax.experimental.pallas import tpu as pltpu
from jax.sharding import PartitionSpec as P

THERMAL = 0.2
HALINE = 0.8
REDI = 0.1
SKEW = 0.05
SLOPE_MAX = 0.6
SLOPE_WIDTH = 0.2
FACE = 0.25 * (REDI - SKEW)
LEVEL = 0.25 * (REDI + SKEW) / REDI
LOADS = (0.5, 1.0)
STORES = (0.2, 0.4, 0.6, 0.8, 1.0)
UNROLL = 4
EVEN = (1, 5)
ODD = (5, 6)


def taper(slope):
    return slope * 0.5 * (1.0 + jnp.tanh((SLOPE_MAX - jnp.abs(slope)) * (1.0 / SLOPE_WIDTH)))


def lanes_of(shape):
    return lax.broadcasted_iota(jnp.int32, shape, len(shape) - 1)


def rows_of(shape):
    return lax.broadcasted_iota(jnp.int32, shape, len(shape) - 2)


def density_of(heat, salt):
    return HALINE * salt - THERMAL * heat


def as_mask(flag):
    return jnp.where(flag, 1.0, 0.0)


def slope_at(here, there, mask, strat_here, strat_there):
    return taper((here - there) * mask / jnp.maximum(0.5 * (strat_here + strat_there), 1.0))


def level_lists(values, masks):
    diffs = [(values[k + 1] - values[k]) * masks[k] for k in range(len(values) - 1)]
    sums = [diffs[0]] + [a + b for a, b in zip(diffs, diffs[1:])] + [diffs[-1]]
    return diffs, sums


def level_rows(values, mask):
    diffs = (pltpu.roll(values, values.shape[0] - 1, 0) - values) * mask
    return diffs, diffs + pltpu.roll(diffs, 1, 0)


def position():
    lat = lax.axis_index("lat")
    return lax.rem(lat, 2) == 1, lat == 0, lat == lax.axis_size("lat") - 1


def pick(values, index):
    return jnp.take_along_axis(values, index, axis=1, mode="promise_in_bounds")


def pair_of(west, east, cols=128):
    shape = (west.shape[0], cols)
    return jnp.where(lax.rem(lanes_of(shape), 2) == 0, jnp.broadcast_to(west, shape), jnp.broadcast_to(east, shape))


def pack_kernel(dims, x_hbm, kmt_hbm, x_ref, own_ref, east_ref, west_ref, kmt_ref, even_ref, odd_ref, raw_ref, sems):
    nt, nz, rows, cols, mirror_color = dims
    per = cols // nt
    bounds = chunk_bounds(nt, LOADS)
    kmt_copy = pltpu.make_async_copy(kmt_hbm, raw_ref, sems.at[len(bounds)])
    kmt_copy.start()
    copies = []
    for c, (first, last) in enumerate(bounds):
        part = pl.ds(first * nz * rows, (last - first) * nz * rows)
        copies.append(pltpu.make_async_copy(x_hbm.at[part], x_ref.at[part], sems.at[c]))
        copies[-1].start()
    shape = (rows, cols)
    lane = lanes_of(shape)
    odd, _, top = position()

    def put_rows(low, high, start):
        index = lanes_of(low.shape)
        turned = pick(high, jnp.where(top, cols - 1 - index, index))
        for color, ref in ((0, even_ref), (1, odd_ref)):
            up = turned if color == mirror_color else high
            goes_up = odd if color == 1 else jnp.logical_not(odd)
            ref[pl.ds(start, nz), :] = jnp.where(goes_up, up, low)

    pairs = [jnp.zeros(shape, jnp.float32)] * nz
    for c, (first, last) in enumerate(bounds):
        copies[c].wait()
        for t in range(first, last):
            here = (lane == 2 * t) | (lane == (2 * t - 1) % cols)
            for k in range(nz):
                value = x_ref[pl.ds((t * nz + k) * rows, rows), :]
                pairs[k] = jnp.where(here, pltpu.roll(value, 2 * t, 1) if t else value, pairs[k])
        for t in range(first, last):
            start = t * nz * rows
            put_rows(x_ref[pl.ds(start, nz, stride=rows), :], x_ref[pl.ds(start + rows - 1, nz, stride=rows), :], t * nz)
    kmt_copy.wait()
    kmt = raw_ref[...].astype(jnp.float32)
    kmt_ref[...] = kmt
    put_rows(jnp.broadcast_to(kmt[:1], (nz, cols)), jnp.broadcast_to(kmt[rows - 1 :], (nz, cols)), nt * nz)
    for k in range(nz):
        own_ref[pl.ds(k * rows, rows), :] = pairs[k]
    for j in range(nz // per + 1):
        east = west = jnp.zeros(shape, jnp.float32)
        for i in range(per):
            k, start = j * per + i, i * nt
            if k > nz:
                break
            index = lax.rem(2 * (lane - start + cols), cols)
            if k == nz:
                side = (jnp.broadcast_to(kmt[:, cols - 1 :], shape), jnp.broadcast_to(kmt[:, :1], shape))
            else:
                side = pick(pairs[k], lax.rem(index + cols - 1, cols)), pick(pairs[k], index)
            east, west = (jnp.where(lane >= start, a, b) for a, b in zip(side, (east, west)))
        east_ref[pl.ds(j * rows, rows), :] = east
        west_ref[pl.ds(j * rows, rows), :] = west


def chunk_bounds(nt, shares):
    ends = [round(nt * share) for share in shares]
    return list(zip([0] + ends, ends))


def pairs_of(west_ref, east_ref, dims, count):
    nt, _, rows, cols, _ = dims
    per = cols // nt
    lane = lanes_of((rows, cols))
    even = lax.rem(lane, 2) == 0
    slot = jnp.where(even, lane // 2, lax.rem(lane + 1, cols) // 2)
    pairs = []
    for k in range(count):
        index = lax.rem(slot + (k % per) * nt, cols)
        part = pl.ds((k // per) * rows, rows)
        pairs.append(jnp.where(even, pick(west_ref[part, :], index), pick(east_ref[part, :], index)))
    return pairs


def early_blocks():
    odd, _, top = position()
    first = (lax.axis_index("lon") == 0) & jnp.logical_not(top)
    return tuple(jnp.where(first, jnp.where(odd, b, a), 0) for a, b in zip(EVEN, ODD))


def early_kernel(dims, x_ref, kmt_ref, *refs):
    *refs, turned_ref = refs
    early, _ = early_blocks()

    @pl.when(early > 0)
    def _():
        coefs_body(dims, x_ref, kmt_ref, *refs[2:])
        inner_body(dims, 0, early, turned_ref, x_ref, kmt_ref, *refs)


def middle_kernel(dims, x_ref, kmt_ref, *refs):
    *refs, turned_ref = refs
    refs = refs[len(refs) // 2 :]
    early, done = early_blocks()

    @pl.when((early == 0) & (done > 0))
    def _():
        coefs_body(dims, x_ref, kmt_ref, *refs[2:])

    inner_body(dims, early, done, turned_ref, x_ref, kmt_ref, *refs)


def late_kernel(dims, x_ref, kmt_ref, *refs):
    *refs, turned_ref = refs
    refs = refs[len(refs) // 2 :]
    _, done = early_blocks()

    @pl.when(done == 0)
    def _():
        coefs_body(dims, x_ref, kmt_ref, *refs[2:])

    inner_body(dims, done, dims[0] // UNROLL, turned_ref, x_ref, kmt_ref, *refs)


def coefs_body(dims, x_ref, kmt_ref, sum_y_ref, inner_ref, dense_ref, cell_w_ref, cell_e_ref, ax_ref, bx_ref, ay_ref, by_ref, p_ref, pw_ref, q_ref, z_ref):
    _, nz, rows, cols, _ = dims
    shape = (rows, cols)
    lane, row = lanes_of(shape), rows_of(shape)
    kmt = kmt_ref[...]
    heat = [x_ref[pl.ds(k * rows, rows), :] for k in range(nz)]
    salt = [x_ref[pl.ds((nz + k) * rows, rows), :] for k in range(nz)]
    density = [density_of(h, s) for h, s in zip(heat, salt)]
    wm = [as_mask(kmt > k + 1) for k in range(nz - 1)]
    kmt_w = pltpu.roll(kmt, 1, 1)
    strat = [0.5 * s for s in level_lists(density, wm)[1]]
    kmt_x = jnp.where(lane == 0, 0.0, jnp.minimum(kmt, kmt_w))
    kmt_y = jnp.where(row == 0, 0.0, jnp.minimum(kmt, pltpu.roll(kmt, 1, 0)))
    sum_x, sum_y = [], []
    for k in range(nz):
        part = pl.ds(k * rows, rows)
        mask = as_mask(kmt_x > k)
        slope = slope_at(density[k], pltpu.roll(density[k], 1, 1), mask, strat[k], pltpu.roll(strat[k], 1, 1))
        ax_ref[part, :] = REDI * mask
        bx_ref[part, :] = FACE * slope
        sum_x.append(slope + pltpu.roll(slope, cols - 1, 1))
        inner_ref[part, :] = pair_of(slope[:, 1:2], slope[:, cols - 1 :])
        mask = as_mask(kmt_y > k)
        slope = slope_at(density[k], pltpu.roll(density[k], 1, 0), mask, strat[k], pltpu.roll(strat[k], 1, 0))
        ay_ref[part, :] = REDI * mask
        by_ref[part, :] = FACE * slope
        sum_y.append(slope + pltpu.roll(slope, rows - 1, 0))
        sum_y_ref[part, :] = sum_y[k]
        dense_ref[part, :] = pair_of(density[k][:, :1], density[k][:, cols - 1 :])
        cell_w_ref[part, :] = jnp.zeros(shape, jnp.float32)
        cell_e_ref[part, :] = jnp.zeros(shape, jnp.float32)
    for k in range(nz - 1):
        part = pl.ds(k * rows, rows)
        level_x, level_y = 0.25 * (sum_x[k] + sum_x[k + 1]), 0.25 * (sum_y[k] + sum_y[k + 1])
        p = LEVEL * level_x * wm[k]
        p_ref[part, :] = p
        pw_ref[part, :] = pltpu.roll(p, 1, 1)
        q_ref[part, :] = LEVEL * level_y * wm[k]
        z_ref[part, :] = REDI * (level_x * level_x + level_y * level_y) * wm[k]


def inner_body(dims, first, last, turned_ref, x_ref, kmt_ref, base_ref, cy_ref, sum_y_ref, inner_ref, dense_ref, cell_w_ref, cell_e_ref,
               ax_ref, bx_ref, ay_ref, by_ref, p_ref, pw_ref, q_ref, z_ref):
    nt, nz, rows, cols, _ = dims
    lane = lanes_of((rows, cols))

    def load(ref, k):
        return ref[pl.ds(k * rows, rows), :]

    def turn(i):
        for j in range(UNROLL * nz):
            part = pl.ds(pl.multiple_of((i * UNROLL * nz + j) * rows, rows), rows)
            turned_ref[lax.rem(i, 2), pl.ds(j * rows, rows), :] = pltpu.roll(x_ref[part, :], 1, 1)

    def tracer(i, j, wm, wm_w):
        t = i * UNROLL + j
        base = t * (nz * rows)
        part = lambda k: pl.ds(pl.multiple_of(base + k * rows, rows), rows)
        value = [x_ref[part(k), :] for k in range(nz)]
        beside = [turned_ref[lax.rem(i, 2), pl.ds((j * nz + k) * rows, rows), :] for k in range(nz)]
        diff, total = level_lists(value, wm)
        total_w = level_lists(beside, wm_w)[1]
        at_east, at_west = lane == lax.rem(2 * t + cols - 1, cols), lane == 2 * t + 1
        new, grads, fluxes, cell_y = [], [], [], []
        for k in range(nz):
            grad = load(ax_ref, k) * (value[k] - beside[k])
            grads.append(grad)
            fluxes.append(grad + load(bx_ref, k) * (total[k] + total_w[k]))
            grad = load(ay_ref, k) * (value[k] - pltpu.roll(value[k], 1, 0))
            flux = grad + load(by_ref, k) * (total[k] + pltpu.roll(total[k], 1, 0))
            cell_y.append(grad + pltpu.roll(grad, rows - 1, 0))
            new.append((value[k] - fluxes[k]) + (pltpu.roll(flux, rows - 1, 0) - flux))
        down = down_w = None
        for k in range(nz):
            result, west = new[k], fluxes[k]
            if k > 0:
                result, west = result - down, west - down_w
            if k < nz - 1:
                both_x, both_y = grads[k] + grads[k + 1], cell_y[k] + cell_y[k + 1]
                down = load(p_ref, k) * both_x + load(q_ref, k) * both_y + load(z_ref, k) * diff[k]
                down_w = load(pw_ref, k) * both_x
                result, west = result + down, west + down_w
                cy_ref[part(k), :] = both_y
                moved = pltpu.roll(both_x, lax.rem(2 * t, cols), 1)
                cell_e_ref[pl.ds(k * rows, rows), :] = jnp.where(at_east, moved, load(cell_e_ref, k))
                cell_w_ref[pl.ds(k * rows, rows), :] = jnp.where(at_west, moved, load(cell_w_ref, k))
            else:
                cy_ref[part(k), :] = jnp.zeros((rows, cols), jnp.float32)
            base_ref[part(k), :] = result + pltpu.roll(west, cols - 1, 1)

    @pl.when(first < last)
    def _():
        kmt = kmt_ref[...]
        kmt_w = pltpu.roll(kmt, 1, 1)
        wm = [as_mask(kmt > k + 1) for k in range(nz - 1)]
        wm_w = [as_mask(kmt_w > k + 1) for k in range(nz - 1)]
        turn(first)

        def step(i, carry):
            for j in range(UNROLL):
                tracer(i, j, wm, wm_w)
            turn(jnp.minimum(i + 1, nt // UNROLL - 1))
            return carry

        lax.fori_loop(first, last, step, 0)


def rows_kernel(dims, x_ref, kmt_ref, base_ref, cy_ref, sum_y_ref, even_ref, odd_ref, out_ref):
    nt, nz, rows, cols, _ = dims
    odd, bottom, _ = position()
    kmt = kmt_ref[...]
    flat = (nz, cols)
    level = rows_of(flat).astype(jnp.float32)

    def ends(index):
        a, b = even_ref[pl.ds(index, nz), :], odd_ref[pl.ds(index, nz), :]
        return jnp.where(odd, a, b), jnp.where(odd, b, a)

    def own_rows(ref, t):
        start = t * nz * rows
        return ref[pl.ds(start, nz, stride=rows), :], ref[pl.ds(start + rows - 1, nz, stride=rows), :]

    ghost_kmts = ends(nt * nz)
    ghost_kmts = jnp.where(bottom, 0.0, ghost_kmts[0]), ghost_kmts[1]
    own_kmts = jnp.broadcast_to(kmt[:1], flat), jnp.broadcast_to(kmt[rows - 1 :], flat)
    heats, salts = (own_rows(x_ref, 0), ends(0)), (own_rows(x_ref, 1), ends(nz))
    sums_before = own_rows(sum_y_ref, 0)
    end_coefs = []
    for end, sign in ((0, -1.0), (1, 1.0)):
        kmts = own_kmts[end], ghost_kmts[end]
        wms = [as_mask(k > level + 1.0) for k in kmts]
        mask = as_mask(jnp.minimum(*kmts) > level)
        densities = [density_of(h[end], s[end]) for h, s in zip(heats, salts)]
        strats = [0.5 * level_rows(d, m)[1] for d, m in zip(densities, wms)]
        slope = sign * slope_at(densities[1], densities[0], mask, *strats)
        before = 0.25 * (sums_before[end] + pltpu.roll(sums_before[end], nz - 1, 0))
        change = 0.25 * (slope + pltpu.roll(slope, nz - 1, 0))
        after = before + change
        own_wm = wms[0]
        end_coefs.append((wms, REDI * mask, sign * FACE * slope, sign * LEVEL * after * own_wm, LEVEL * change * own_wm,
                          REDI * change * (before + after) * own_wm))
    for t in range(nt):
        for end in (0, 1):
            wms, a, b, q, q_change, z_change = end_coefs[end]
            here, there = own_rows(x_ref, t)[end], ends(t * nz)[end]
            diff, own_sum = level_rows(here, wms[0])
            grad = a * (there - here)
            gain = grad + b * (own_sum + level_rows(there, wms[1])[1])
            tilt = q * (grad + pltpu.roll(grad, nz - 1, 0)) + q_change * own_rows(cy_ref, t)[end] + z_change * diff
            part = pl.ds(t * nz * rows + (rows - 1 if end else 0), nz, stride=rows)
            out_ref[part, :] = out_ref[part, :] + (gain + (tilt - pltpu.roll(tilt, 1, 0)))


def outer_kernel(dims, kmt_ref, own_ref, base_ref, inner_ref, dense_ref, cell_w_ref, cell_e_ref,
                 from_west, from_east, out_hbm, out_ref, side_ref, sems):
    nt, nz, rows, cols, _ = dims
    shape = (rows, cols)
    lane = lanes_of(shape)
    per = cols // nt
    even = lax.rem(lane, 2) == 0
    kmt = kmt_ref[...]

    def load(ref, k):
        return ref[pl.ds(k * rows, rows), :]

    def spread(k, t):
        start = (k % per) * nt + t
        return pair_of(load(from_west, k // per)[:, start : start + 1], load(from_east, k // per)[:, start : start + 1])

    outward = jnp.where(even, -1.0, 1.0)
    own = [load(own_ref, k) for k in range(nz)]
    ghost = pairs_of(from_west, from_east, dims, nz)
    own_kmt, ghost_kmt = pair_of(kmt[:, :1], kmt[:, cols - 1 :]), spread(nz, 0)
    own_density = [load(dense_ref, k) for k in range(nz)]
    ghost_density = [density_of(spread(k, 0), spread(k, 1)) for k in range(nz)]
    own_wm = [as_mask(own_kmt > k + 1) for k in range(nz - 1)]
    ghost_wm = [as_mask(ghost_kmt > k + 1) for k in range(nz - 1)]
    side_mask = [as_mask(jnp.minimum(own_kmt, ghost_kmt) > k) for k in range(nz)]
    own_strat = level_lists(own_density, own_wm)[1]
    ghost_strat = level_lists(ghost_density, ghost_wm)[1]
    side_slope = [
        outward * slope_at(ghost_density[k], own_density[k], side_mask[k], 0.5 * own_strat[k], 0.5 * ghost_strat[k])
        for k in range(nz)
    ]
    own_diff, own_sum = level_lists(own, own_wm)
    ghost_sum = level_lists(ghost, ghost_wm)[1]
    grad = [REDI * side_mask[k] * (ghost[k] - own[k]) for k in range(nz)]
    flux = [grad[k] + outward * FACE * side_slope[k] * (own_sum[k] + ghost_sum[k]) for k in range(nz)]
    tilt = []
    for k in range(nz - 1):
        before = 0.25 * (load(inner_ref, k) + load(inner_ref, k + 1))
        change = 0.25 * (side_slope[k] + side_slope[k + 1])
        after = before + change
        inner = jnp.where(even, pltpu.roll(load(cell_w_ref, k), cols - 1, 1), load(cell_e_ref, k))
        across = after * outward * (grad[k] + grad[k + 1]) + change * inner
        along = change * (before + after) * own_diff[k]
        tilt.append(own_wm[k] * (LEVEL * across + REDI * along))
    for k in range(nz):
        added = flux[k]
        if k < nz - 1:
            added = added + tilt[k]
        if k > 0:
            added = added - tilt[k - 1]
        side_ref[pl.ds(k * rows, rows), :] = added
    outer = (lane == 0) | (lane == cols - 1)
    copies = []
    for c, (first, last) in enumerate(chunk_bounds(nt, STORES)):
        for t in range(first, last):
            for k in range(nz):
                part = pl.ds((t * nz + k) * rows, rows)
                side = load(side_ref, k)
                side = pltpu.roll(side, cols - 2 * t, 1) if t else side
                out_ref[part, :] = base_ref[part, :] + jnp.where(outer, side, 0.0)
        part = pl.ds(first * nz * rows, (last - first) * nz * rows)
        copies.append(pltpu.make_async_copy(out_ref.at[part], out_hbm.at[part], sems.at[c]))
        copies[-1].start()
    for copy in copies:
        copy.wait()


def idle_partner(lon, lons):
    if lons % 8 == 0 and (lon * 4 // lons) % 2 == 1:
        return (lon + lons // 2) % lons
    return lon ^ 1 if lons % 2 == 0 else lon


def row_pairs(color, lons, lats):
    pairs = []
    for lon in range(lons):
        for lat in range(lats - 1):
            if lat % 2 == color:
                pairs += [(lon * lats + lat, lon * lats + lat + 1), (lon * lats + lat + 1, lon * lats + lat)]
        if (lats - 1) % 2 == color:
            pairs.append((lon * lats + lats - 1, (lons - 1 - lon) * lats + lats - 1))
    free_in = sorted(set(range(lons * lats)) - {b for _, b in pairs})
    free_out = set(range(lons * lats)) - {a for a, _ in pairs}
    for target in free_in:
        lon, lat = divmod(target, lats)
        source = idle_partner(lon, lons) * lats + lat
        assert source in free_out
        pairs.append((source, target))
    return pairs


def local(tracers, kmt):
    nt, nz, rows, cols = tracers.shape
    lons, lats = lax.axis_size("lon"), lax.axis_size("lat")
    dims = (nt, nz, rows, cols, (lats - 1) % 2)
    packed = ((nz // (cols // nt) + 1) * rows, cols)
    edge = (nt * nz + nz, cols)
    level, block = (nz * rows, cols), (nt * nz * rows, cols)
    vmem, anywhere = pl.BlockSpec(memory_space=pltpu.VMEM), pl.BlockSpec(memory_space=pl.ANY)

    def call(kernel, inputs, out_shape, scratch, flops, specs=None, aliases={}):
        out = [pltpu.VMEM(s, jnp.float32) for s in out_shape] if specs is None else out_shape
        if specs is None:
            specs = [vmem] * len(out_shape)
        near = [pltpu.with_memory_space_constraint(a, pltpu.HBM if a is x or a is kmt else pltpu.VMEM) for a in inputs]
        return pl.pallas_call(
            functools.partial(kernel, dims),
            out_shape=out,
            in_specs=[anywhere if a is x or a is kmt else vmem for a in inputs],
            out_specs=specs,
            scratch_shapes=scratch,
            input_output_aliases=aliases,
            cost_estimate=pl.CostEstimate(flops=flops, bytes_accessed=flops, transcendentals=0),
            compiler_params=pltpu.CompilerParams(vmem_limit_bytes=16 * 2**20),
        )(*near)

    x = tracers.reshape(block)
    near, own, east, west, near_kmt, even, odd = call(
        pack_kernel,
        (x, kmt),
        (block, level, packed, packed, (rows, cols), edge, edge),
        [pltpu.VMEM((rows, cols), jnp.int32), pltpu.SemaphoreType.DMA((len(LOADS) + 1,))],
        1000000,
    )
    ring = [(i, (i + 1) % lons) for i in range(lons)]
    from_west = lax.ppermute(east, "lon", ring)
    shapes = (block,) * 2 + (level,) * 13
    turned = [pltpu.VMEM((2, UNROLL * nz * rows, cols), jnp.float32)]
    inner = call(early_kernel, (near, near_kmt), shapes, turned, 10000000)
    from_odd = lax.ppermute(odd, ("lon", "lat"), row_pairs(1, lons, lats))
    aliases = {2 + i: i for i in range(len(shapes))}
    inner = call(middle_kernel, (near, near_kmt, *inner), shapes, turned, 10000000, aliases=aliases)
    from_even = lax.ppermute(even, ("lon", "lat"), row_pairs(0, lons, lats))
    from_east = lax.ppermute(west, "lon", [(b, a) for a, b in ring])
    inner = call(late_kernel, (near, near_kmt, *inner), shapes, turned, 10000000, aliases=aliases)
    base, cy, sum_y, inner_slope, dense, cell_w, cell_e = inner[:7]
    ends = (near, near_kmt, base, cy, sum_y, from_even, from_odd)
    (base,) = call(rows_kernel, ends, (block,), [], 1000000, aliases={2: 0})
    out = call(
        outer_kernel,
        (near_kmt, own, base, inner_slope, dense, cell_w, cell_e, from_west, from_east),
        jax.ShapeDtypeStruct(block, jnp.float32),
        [pltpu.VMEM(block, jnp.float32), pltpu.VMEM(level, jnp.float32), pltpu.SemaphoreType.DMA((len(STORES),))],
        10000000,
        anywhere,
    )
    return out.reshape(tracers.shape)


def solution(mesh):
    return jax.shard_map(
        local,
        mesh=mesh,
        in_specs=(P(None, None, "lat", "lon"), P("lat", "lon")),
        out_specs=P(None, None, "lat", "lon"),
        check_vma=False,
    )
```

```python
import functools

import jax
import jax.numpy as jnp
from jax import lax
from jax.experimental import pallas as pl
from jax.experimental.pallas import tpu as pltpu
from jax.sharding import PartitionSpec as P

THERMAL = 0.2
HALINE = 0.8
REDI = 0.1
SKEW = 0.05
SLOPE_MAX = 0.6
SLOPE_WIDTH = 0.2
FACE = 0.25 * (REDI - SKEW)
LEVEL = 0.25 * (REDI + SKEW) / REDI
LOADS = (0.5, 1.0)
STORES = (0.2, 0.4, 0.6, 0.8, 1.0)
UNROLL = 4
EVEN = (1, 5)
ODD = (5, 6)


def taper(slope):
    return slope * 0.5 * (1.0 + jnp.tanh((SLOPE_MAX - jnp.abs(slope)) * (1.0 / SLOPE_WIDTH)))


def lanes_of(shape):
    return lax.broadcasted_iota(jnp.int32, shape, len(shape) - 1)


def rows_of(shape):
    return lax.broadcasted_iota(jnp.int32, shape, len(shape) - 2)


def density_of(heat, salt):
    return HALINE * salt - THERMAL * heat


def as_mask(flag):
    return jnp.where(flag, 1.0, 0.0)


def slope_at(here, there, mask, strat_here, strat_there):
    return taper((here - there) * mask / jnp.maximum(0.5 * (strat_here + strat_there), 1.0))


def level_lists(values, masks):
    diffs = [(values[k + 1] - values[k]) * masks[k] for k in range(len(values) - 1)]
    sums = [diffs[0]] + [a + b for a, b in zip(diffs, diffs[1:])] + [diffs[-1]]
    return diffs, sums


def level_rows(values, mask):
    diffs = (pltpu.roll(values, values.shape[0] - 1, 0) - values) * mask
    return diffs, diffs + pltpu.roll(diffs, 1, 0)


def position():
    lat = lax.axis_index("lat")
    return lax.rem(lat, 2) == 1, lat == 0, lat == lax.axis_size("lat") - 1


def pick(values, index):
    return jnp.take_along_axis(values, index, axis=1, mode="promise_in_bounds")


def pair_of(west, east, cols=128):
    shape = (west.shape[0], cols)
    return jnp.where(lax.rem(lanes_of(shape), 2) == 0, jnp.broadcast_to(west, shape), jnp.broadcast_to(east, shape))


def pack_kernel(dims, x_hbm, kmt_hbm, x_ref, own_ref, east_ref, west_ref, kmt_ref, even_ref, odd_ref, raw_ref, sems):
    nt, nz, rows, cols, mirror_color = dims
    per = cols // nt
    bounds = chunk_bounds(nt, LOADS)
    kmt_copy = pltpu.make_async_copy(kmt_hbm, raw_ref, sems.at[len(bounds)])
    kmt_copy.start()
    copies = []
    for c, (first, last) in enumerate(bounds):
        part = pl.ds(first * nz * rows, (last - first) * nz * rows)
        copies.append(pltpu.make_async_copy(x_hbm.at[part], x_ref.at[part], sems.at[c]))
        copies[-1].start()
    shape = (rows, cols)
    lane = lanes_of(shape)
    odd, _, top = position()

    def put_rows(low, high, start):
        index = lanes_of(low.shape)
        turned = pick(high, jnp.where(top, cols - 1 - index, index))
        for color, ref in ((0, even_ref), (1, odd_ref)):
            up = turned if color == mirror_color else high
            goes_up = odd if color == 1 else jnp.logical_not(odd)
            ref[pl.ds(start, nz), :] = jnp.where(goes_up, up, low)

    pairs = [jnp.zeros(shape, jnp.float32)] * nz
    for c, (first, last) in enumerate(bounds):
        copies[c].wait()
        for t in range(first, last):
            here = (lane == 2 * t) | (lane == (2 * t - 1) % cols)
            for k in range(nz):
                value = x_ref[pl.ds((t * nz + k) * rows, rows), :]
                pairs[k] = jnp.where(here, pltpu.roll(value, 2 * t, 1) if t else value, pairs[k])
        for t in range(first, last):
            start = t * nz * rows
            put_rows(x_ref[pl.ds(start, nz, stride=rows), :], x_ref[pl.ds(start + rows - 1, nz, stride=rows), :], t * nz)
    kmt_copy.wait()
    kmt = raw_ref[...].astype(jnp.float32)
    kmt_ref[...] = kmt
    put_rows(jnp.broadcast_to(kmt[:1], (nz, cols)), jnp.broadcast_to(kmt[rows - 1 :], (nz, cols)), nt * nz)
    for k in range(nz):
        own_ref[pl.ds(k * rows, rows), :] = pairs[k]
    for j in range(nz // per + 1):
        east = west = jnp.zeros(shape, jnp.float32)
        for i in range(per):
            k, start = j * per + i, i * nt
            if k > nz:
                break
            index = lax.rem(2 * (lane - start + cols), cols)
            if k == nz:
                side = (jnp.broadcast_to(kmt[:, cols - 1 :], shape), jnp.broadcast_to(kmt[:, :1], shape))
            else:
                side = pick(pairs[k], lax.rem(index + cols - 1, cols)), pick(pairs[k], index)
            east, west = (jnp.where(lane >= start, a, b) for a, b in zip(side, (east, west)))
        east_ref[pl.ds(j * rows, rows), :] = east
        west_ref[pl.ds(j * rows, rows), :] = west


def chunk_bounds(nt, shares):
    ends = [round(nt * share) for share in shares]
    return list(zip([0] + ends, ends))


def pairs_of(west_ref, east_ref, dims, count):
    nt, _, rows, cols, _ = dims
    per = cols // nt
    lane = lanes_of((rows, cols))
    even = lax.rem(lane, 2) == 0
    slot = jnp.where(even, lane // 2, lax.rem(lane + 1, cols) // 2)
    pairs = []
    for k in range(count):
        index = lax.rem(slot + (k % per) * nt, cols)
        part = pl.ds((k // per) * rows, rows)
        pairs.append(jnp.where(even, pick(west_ref[part, :], index), pick(east_ref[part, :], index)))
    return pairs


def early_blocks():
    odd, _, top = position()
    first = (lax.axis_index("lon") == 0) & jnp.logical_not(top)
    return tuple(jnp.where(first, jnp.where(odd, b, a), 0) for a, b in zip(EVEN, ODD))


def early_kernel(dims, x_ref, kmt_ref, *refs):
    *refs, turned_ref = refs
    early, _ = early_blocks()

    @pl.when(early > 0)
    def _():
        coefs_body(dims, x_ref, kmt_ref, *refs[2:])
        inner_body(dims, 0, early, turned_ref, x_ref, kmt_ref, *refs)


def middle_kernel(dims, x_ref, kmt_ref, *refs):
    *refs, turned_ref = refs
    refs = refs[len(refs) // 2 :]
    early, done = early_blocks()

    @pl.when((early == 0) & (done > 0))
    def _():
        coefs_body(dims, x_ref, kmt_ref, *refs[2:])

    inner_body(dims, early, done, turned_ref, x_ref, kmt_ref, *refs)


def late_kernel(dims, x_ref, kmt_ref, *refs):
    *refs, turned_ref = refs
    refs = refs[len(refs) // 2 :]
    _, done = early_blocks()

    @pl.when(done == 0)
    def _():
        coefs_body(dims, x_ref, kmt_ref, *refs[2:])

    inner_body(dims, done, dims[0] // UNROLL, turned_ref, x_ref, kmt_ref, *refs)


def coefs_body(dims, x_ref, kmt_ref, sum_y_ref, inner_ref, dense_ref, cell_w_ref, cell_e_ref, ax_ref, bx_ref, ay_ref, by_ref, p_ref, pw_ref, q_ref, z_ref):
    _, nz, rows, cols, _ = dims
    shape = (rows, cols)
    lane, row = lanes_of(shape), rows_of(shape)
    kmt = kmt_ref[...]
    heat = [x_ref[pl.ds(k * rows, rows), :] for k in range(nz)]
    salt = [x_ref[pl.ds((nz + k) * rows, rows), :] for k in range(nz)]
    density = [density_of(h, s) for h, s in zip(heat, salt)]
    wm = [as_mask(kmt > k + 1) for k in range(nz - 1)]
    kmt_w = pltpu.roll(kmt, 1, 1)
    strat = [0.5 * s for s in level_lists(density, wm)[1]]
    kmt_x = jnp.where(lane == 0, 0.0, jnp.minimum(kmt, kmt_w))
    kmt_y = jnp.where(row == 0, 0.0, jnp.minimum(kmt, pltpu.roll(kmt, 1, 0)))
    sum_x, sum_y = [], []
    for k in range(nz):
        part = pl.ds(k * rows, rows)
        mask = as_mask(kmt_x > k)
        slope = slope_at(density[k], pltpu.roll(density[k], 1, 1), mask, strat[k], pltpu.roll(strat[k], 1, 1))
        ax_ref[part, :] = REDI * mask
        bx_ref[part, :] = FACE * slope
        sum_x.append(slope + pltpu.roll(slope, cols - 1, 1))
        inner_ref[part, :] = pair_of(slope[:, 1:2], slope[:, cols - 1 :])
        mask = as_mask(kmt_y > k)
        slope = slope_at(density[k], pltpu.roll(density[k], 1, 0), mask, strat[k], pltpu.roll(strat[k], 1, 0))
        ay_ref[part, :] = REDI * mask
        by_ref[part, :] = FACE * slope
        sum_y.append(slope + pltpu.roll(slope, rows - 1, 0))
        sum_y_ref[part, :] = sum_y[k]
        dense_ref[part, :] = pair_of(density[k][:, :1], density[k][:, cols - 1 :])
        cell_w_ref[part, :] = jnp.zeros(shape, jnp.float32)
        cell_e_ref[part, :] = jnp.zeros(shape, jnp.float32)
    for k in range(nz - 1):
        part = pl.ds(k * rows, rows)
        level_x, level_y = 0.25 * (sum_x[k] + sum_x[k + 1]), 0.25 * (sum_y[k] + sum_y[k + 1])
        p = LEVEL * level_x * wm[k]
        p_ref[part, :] = p
        pw_ref[part, :] = pltpu.roll(p, 1, 1)
        q_ref[part, :] = LEVEL * level_y * wm[k]
        z_ref[part, :] = REDI * (level_x * level_x + level_y * level_y) * wm[k]


def inner_body(dims, first, last, turned_ref, x_ref, kmt_ref, base_ref, cy_ref, sum_y_ref, inner_ref, dense_ref, cell_w_ref, cell_e_ref,
               ax_ref, bx_ref, ay_ref, by_ref, p_ref, pw_ref, q_ref, z_ref):
    nt, nz, rows, cols, _ = dims
    lane = lanes_of((rows, cols))

    def load(ref, k):
        return ref[pl.ds(k * rows, rows), :]

    def turn(i):
        for j in range(UNROLL * nz):
            part = pl.ds(pl.multiple_of((i * UNROLL * nz + j) * rows, rows), rows)
            turned_ref[lax.rem(i, 2), pl.ds(j * rows, rows), :] = pltpu.roll(x_ref[part, :], 1, 1)

    def tracer(i, j, wm, wm_w):
        t = i * UNROLL + j
        base = t * (nz * rows)
        part = lambda k: pl.ds(pl.multiple_of(base + k * rows, rows), rows)
        value = [x_ref[part(k), :] for k in range(nz)]
        beside = [turned_ref[lax.rem(i, 2), pl.ds((j * nz + k) * rows, rows), :] for k in range(nz)]
        diff, total = level_lists(value, wm)
        total_w = level_lists(beside, wm_w)[1]
        at_east, at_west = lane == lax.rem(2 * t + cols - 1, cols), lane == 2 * t + 1
        new, grads, fluxes, cell_y = [], [], [], []
        for k in range(nz):
            grad = load(ax_ref, k) * (value[k] - beside[k])
            grads.append(grad)
            fluxes.append(grad + load(bx_ref, k) * (total[k] + total_w[k]))
            grad = load(ay_ref, k) * (value[k] - pltpu.roll(value[k], 1, 0))
            flux = grad + load(by_ref, k) * (total[k] + pltpu.roll(total[k], 1, 0))
            cell_y.append(grad + pltpu.roll(grad, rows - 1, 0))
            new.append((value[k] - fluxes[k]) + (pltpu.roll(flux, rows - 1, 0) - flux))
        down = down_w = None
        for k in range(nz):
            result, west = new[k], fluxes[k]
            if k > 0:
                result, west = result - down, west - down_w
            if k < nz - 1:
                both_x, both_y = grads[k] + grads[k + 1], cell_y[k] + cell_y[k + 1]
                down = load(p_ref, k) * both_x + load(q_ref, k) * both_y + load(z_ref, k) * diff[k]
                down_w = load(pw_ref, k) * both_x
                result, west = result + down, west + down_w
                cy_ref[part(k), :] = both_y
                moved = pltpu.roll(both_x, lax.rem(2 * t, cols), 1)
                cell_e_ref[pl.ds(k * rows, rows), :] = jnp.where(at_east, moved, load(cell_e_ref, k))
                cell_w_ref[pl.ds(k * rows, rows), :] = jnp.where(at_west, moved, load(cell_w_ref, k))
            else:
                cy_ref[part(k), :] = jnp.zeros((rows, cols), jnp.float32)
            base_ref[part(k), :] = result + pltpu.roll(west, cols - 1, 1)

    @pl.when(first < last)
    def _():
        kmt = kmt_ref[...]
        kmt_w = pltpu.roll(kmt, 1, 1)
        wm = [as_mask(kmt > k + 1) for k in range(nz - 1)]
        wm_w = [as_mask(kmt_w > k + 1) for k in range(nz - 1)]
        turn(first)

        def step(i, carry):
            for j in range(UNROLL):
                tracer(i, j, wm, wm_w)
            turn(jnp.minimum(i + 1, nt // UNROLL - 1))
            return carry

        lax.fori_loop(first, last, step, 0)


def end_kernel(color, dims, x_ref, kmt_ref, base_ref, cy_ref, sum_y_ref, there_ref, out_ref):
    nt, nz, rows, cols, _ = dims
    odd, bottom, _ = position()
    north = odd if color == 1 else jnp.logical_not(odd)
    flat = (nz, cols)
    level = rows_of(flat).astype(jnp.float32)

    def side(row, sign):
        def own_row(ref, t):
            return ref[pl.ds(t * nz * rows + row, nz, stride=rows), :]

        def ghost_row(t):
            return there_ref[pl.ds(t * nz, nz), :]

        kmts = jnp.broadcast_to(kmt_ref[row : row + 1, :], flat), ghost_row(nt)
        own_wm, ghost_wm = [as_mask(k > level + 1.0) for k in kmts]
        mask = as_mask(jnp.minimum(*kmts) > level)
        own_density = density_of(own_row(x_ref, 0), own_row(x_ref, 1))
        ghost_density = density_of(ghost_row(0), ghost_row(1))
        own_strat, ghost_strat = level_rows(own_density, own_wm)[1], level_rows(ghost_density, ghost_wm)[1]
        slope = sign * slope_at(ghost_density, own_density, mask, 0.5 * own_strat, 0.5 * ghost_strat)
        before = own_row(sum_y_ref, 0)
        before = 0.25 * (before + pltpu.roll(before, nz - 1, 0))
        change = 0.25 * (slope + pltpu.roll(slope, nz - 1, 0))
        after = before + change
        a, b = REDI * mask, sign * FACE * slope
        q, q_change = sign * LEVEL * after * own_wm, LEVEL * change * own_wm
        z_change = REDI * change * (before + after) * own_wm
        for t in range(nt):
            here, there = own_row(x_ref, t), ghost_row(t)
            diff, own_sum = level_rows(here, own_wm)
            grad = a * (there - here)
            gain = grad + b * (own_sum + level_rows(there, ghost_wm)[1])
            tilt = q * (grad + pltpu.roll(grad, nz - 1, 0)) + q_change * own_row(cy_ref, t) + z_change * diff
            part = pl.ds(t * nz * rows + row, nz, stride=rows)
            out_ref[part, :] = out_ref[part, :] + (gain + (tilt - pltpu.roll(tilt, 1, 0)))

    @pl.when(north)
    def _():
        side(rows - 1, 1.0)

    @pl.when(jnp.logical_not(north | bottom))
    def _():
        side(0, -1.0)


def outer_kernel(dims, kmt_ref, own_ref, base_ref, inner_ref, dense_ref, cell_w_ref, cell_e_ref,
                 from_west, from_east, out_hbm, out_ref, side_ref, sems):
    nt, nz, rows, cols, _ = dims
    shape = (rows, cols)
    lane = lanes_of(shape)
    per = cols // nt
    even = lax.rem(lane, 2) == 0
    kmt = kmt_ref[...]

    def load(ref, k):
        return ref[pl.ds(k * rows, rows), :]

    def spread(k, t):
        start = (k % per) * nt + t
        return pair_of(load(from_west, k // per)[:, start : start + 1], load(from_east, k // per)[:, start : start + 1])

    outward = jnp.where(even, -1.0, 1.0)
    own = [load(own_ref, k) for k in range(nz)]
    ghost = pairs_of(from_west, from_east, dims, nz)
    own_kmt, ghost_kmt = pair_of(kmt[:, :1], kmt[:, cols - 1 :]), spread(nz, 0)
    own_density = [load(dense_ref, k) for k in range(nz)]
    ghost_density = [density_of(spread(k, 0), spread(k, 1)) for k in range(nz)]
    own_wm = [as_mask(own_kmt > k + 1) for k in range(nz - 1)]
    ghost_wm = [as_mask(ghost_kmt > k + 1) for k in range(nz - 1)]
    side_mask = [as_mask(jnp.minimum(own_kmt, ghost_kmt) > k) for k in range(nz)]
    own_strat = level_lists(own_density, own_wm)[1]
    ghost_strat = level_lists(ghost_density, ghost_wm)[1]
    side_slope = [
        outward * slope_at(ghost_density[k], own_density[k], side_mask[k], 0.5 * own_strat[k], 0.5 * ghost_strat[k])
        for k in range(nz)
    ]
    own_diff, own_sum = level_lists(own, own_wm)
    ghost_sum = level_lists(ghost, ghost_wm)[1]
    grad = [REDI * side_mask[k] * (ghost[k] - own[k]) for k in range(nz)]
    flux = [grad[k] + outward * FACE * side_slope[k] * (own_sum[k] + ghost_sum[k]) for k in range(nz)]
    tilt = []
    for k in range(nz - 1):
        before = 0.25 * (load(inner_ref, k) + load(inner_ref, k + 1))
        change = 0.25 * (side_slope[k] + side_slope[k + 1])
        after = before + change
        inner = jnp.where(even, pltpu.roll(load(cell_w_ref, k), cols - 1, 1), load(cell_e_ref, k))
        across = after * outward * (grad[k] + grad[k + 1]) + change * inner
        along = change * (before + after) * own_diff[k]
        tilt.append(own_wm[k] * (LEVEL * across + REDI * along))
    for k in range(nz):
        added = flux[k]
        if k < nz - 1:
            added = added + tilt[k]
        if k > 0:
            added = added - tilt[k - 1]
        side_ref[pl.ds(k * rows, rows), :] = added
    outer = (lane == 0) | (lane == cols - 1)
    copies = []
    for c, (first, last) in enumerate(chunk_bounds(nt, STORES)):
        for t in range(first, last):
            for k in range(nz):
                part = pl.ds((t * nz + k) * rows, rows)
                side = load(side_ref, k)
                side = pltpu.roll(side, cols - 2 * t, 1) if t else side
                out_ref[part, :] = base_ref[part, :] + jnp.where(outer, side, 0.0)
        part = pl.ds(first * nz * rows, (last - first) * nz * rows)
        copies.append(pltpu.make_async_copy(out_ref.at[part], out_hbm.at[part], sems.at[c]))
        copies[-1].start()
    for copy in copies:
        copy.wait()


def idle_partner(lon, lons):
    if lons % 8 == 0 and (lon * 4 // lons) % 2 == 1:
        return (lon + lons // 2) % lons
    return lon ^ 1 if lons % 2 == 0 else lon


def row_pairs(color, lons, lats):
    pairs = []
    for lon in range(lons):
        for lat in range(lats - 1):
            if lat % 2 == color:
                pairs += [(lon * lats + lat, lon * lats + lat + 1), (lon * lats + lat + 1, lon * lats + lat)]
        if (lats - 1) % 2 == color:
            pairs.append((lon * lats + lats - 1, (lons - 1 - lon) * lats + lats - 1))
    free_in = sorted(set(range(lons * lats)) - {b for _, b in pairs})
    free_out = set(range(lons * lats)) - {a for a, _ in pairs}
    for target in free_in:
        lon, lat = divmod(target, lats)
        source = idle_partner(lon, lons) * lats + lat
        assert source in free_out
        pairs.append((source, target))
    return pairs


def local(tracers, kmt):
    nt, nz, rows, cols = tracers.shape
    lons, lats = lax.axis_size("lon"), lax.axis_size("lat")
    dims = (nt, nz, rows, cols, (lats - 1) % 2)
    packed = ((nz // (cols // nt) + 1) * rows, cols)
    edge = (nt * nz + nz, cols)
    level, block = (nz * rows, cols), (nt * nz * rows, cols)
    vmem, anywhere = pl.BlockSpec(memory_space=pltpu.VMEM), pl.BlockSpec(memory_space=pl.ANY)

    def call(kernel, inputs, out_shape, scratch, flops, specs=None, aliases={}):
        out = [pltpu.VMEM(s, jnp.float32) for s in out_shape] if specs is None else out_shape
        if specs is None:
            specs = [vmem] * len(out_shape)
        near = [pltpu.with_memory_space_constraint(a, pltpu.HBM if a is x or a is kmt else pltpu.VMEM) for a in inputs]
        return pl.pallas_call(
            functools.partial(kernel, dims),
            out_shape=out,
            in_specs=[anywhere if a is x or a is kmt else vmem for a in inputs],
            out_specs=specs,
            scratch_shapes=scratch,
            input_output_aliases=aliases,
            cost_estimate=pl.CostEstimate(flops=flops, bytes_accessed=flops, transcendentals=0),
            compiler_params=pltpu.CompilerParams(vmem_limit_bytes=16 * 2**20),
        )(*near)

    x = tracers.reshape(block)
    near, own, east, west, near_kmt, even, odd = call(
        pack_kernel,
        (x, kmt),
        (block, level, packed, packed, (rows, cols), edge, edge),
        [pltpu.VMEM((rows, cols), jnp.int32), pltpu.SemaphoreType.DMA((len(LOADS) + 1,))],
        1000000,
    )
    ring = [(i, (i + 1) % lons) for i in range(lons)]
    from_west = lax.ppermute(east, "lon", ring)
    shapes = (block,) * 2 + (level,) * 13
    turned = [pltpu.VMEM((2, UNROLL * nz * rows, cols), jnp.float32)]
    inner = call(early_kernel, (near, near_kmt), shapes, turned, 10000000)
    from_odd = lax.ppermute(odd, ("lon", "lat"), row_pairs(1, lons, lats))
    aliases = {2 + i: i for i in range(len(shapes))}
    inner = call(middle_kernel, (near, near_kmt, *inner), shapes, turned, 10000000, aliases=aliases)
    from_even = lax.ppermute(even, ("lon", "lat"), row_pairs(0, lons, lats))
    from_east = lax.ppermute(west, "lon", [(b, a) for a, b in ring])
    inner = call(late_kernel, (near, near_kmt, *inner), shapes, turned, 10000000, aliases=aliases)
    base, cy, sum_y, inner_slope, dense, cell_w, cell_e = inner[:7]
    for color, there in ((0, from_even), (1, from_odd)):
        inputs = (near, near_kmt, base, cy, sum_y, there)
        (base,) = call(functools.partial(end_kernel, color), inputs, (block,), [], 1000000, aliases={2: 0})
    out = call(
        outer_kernel,
        (near_kmt, own, base, inner_slope, dense, cell_w, cell_e, from_west, from_east),
        jax.ShapeDtypeStruct(block, jnp.float32),
        [pltpu.VMEM(block, jnp.float32), pltpu.VMEM(level, jnp.float32), pltpu.SemaphoreType.DMA((len(STORES),))],
        10000000,
        anywhere,
    )
    return out.reshape(tracers.shape)


def solution(mesh):
    return jax.shard_map(
        local,
        mesh=mesh,
        in_specs=(P(None, None, "lat", "lon"), P("lat", "lon")),
        out_specs=P(None, None, "lat", "lon"),
        check_vma=False,
    )
```

```python
import functools

import jax
import jax.numpy as jnp
from jax import lax
from jax.experimental import pallas as pl
from jax.experimental.pallas import tpu as pltpu
from jax.sharding import PartitionSpec as P

THERMAL = 0.2
HALINE = 0.8
REDI = 0.1
SKEW = 0.05
SLOPE_MAX = 0.6
SLOPE_WIDTH = 0.2
FACE = 0.25 * (REDI - SKEW)
LEVEL = 0.25 * (REDI + SKEW) / REDI
LOADS = (0.5, 1.0)
STORES = (0.1, 0.2, 0.3, 0.4, 0.5, 0.6, 0.7, 0.8, 0.9, 1.0)
UNROLL = 4
EVEN = (1, 5)
ODD = (5, 6)


def taper(slope):
    return slope * 0.5 * (1.0 + jnp.tanh((SLOPE_MAX - jnp.abs(slope)) * (1.0 / SLOPE_WIDTH)))


def lanes_of(shape):
    return lax.broadcasted_iota(jnp.int32, shape, len(shape) - 1)


def rows_of(shape):
    return lax.broadcasted_iota(jnp.int32, shape, len(shape) - 2)


def density_of(heat, salt):
    return HALINE * salt - THERMAL * heat


def as_mask(flag):
    return jnp.where(flag, 1.0, 0.0)


def slope_at(here, there, mask, strat_here, strat_there):
    return taper((here - there) * mask / jnp.maximum(0.5 * (strat_here + strat_there), 1.0))


def level_lists(values, masks):
    diffs = [(values[k + 1] - values[k]) * masks[k] for k in range(len(values) - 1)]
    sums = [diffs[0]] + [a + b for a, b in zip(diffs, diffs[1:])] + [diffs[-1]]
    return diffs, sums


def level_rows(values, mask):
    diffs = (pltpu.roll(values, values.shape[0] - 1, 0) - values) * mask
    return diffs, diffs + pltpu.roll(diffs, 1, 0)


def position():
    lat = lax.axis_index("lat")
    return lax.rem(lat, 2) == 1, lat == 0, lat == lax.axis_size("lat") - 1


def pick(values, index):
    return jnp.take_along_axis(values, index, axis=1, mode="promise_in_bounds")


def pair_of(west, east, cols):
    shape = (west.shape[0], cols)
    return jnp.where(lax.rem(lanes_of(shape), 2) == 0, jnp.broadcast_to(west, shape), jnp.broadcast_to(east, shape))


def pack_kernel(dims, x_hbm, kmt_hbm, x_ref, own_ref, east_ref, west_ref, kmt_ref, even_ref, odd_ref, raw_ref, sems):
    nt, nz, rows, cols, mirror_color = dims
    per = cols // nt
    bounds = chunk_bounds(nt, LOADS)
    kmt_copy = pltpu.make_async_copy(kmt_hbm, raw_ref, sems.at[len(bounds)])
    kmt_copy.start()
    copies = []
    for c, (first, last) in enumerate(bounds):
        part = pl.ds(first * nz * rows, (last - first) * nz * rows)
        copies.append(pltpu.make_async_copy(x_hbm.at[part], x_ref.at[part], sems.at[c]))
        copies[-1].start()
    shape = (rows, cols)
    lane = lanes_of(shape)
    odd, _, top = position()

    def put_rows(low, high, start):
        index = lanes_of(low.shape)
        turned = pick(high, jnp.where(top, cols - 1 - index, index))
        for color, ref in ((0, even_ref), (1, odd_ref)):
            up = turned if color == mirror_color else high
            goes_up = odd if color == 1 else jnp.logical_not(odd)
            ref[pl.ds(start, nz), :] = jnp.where(goes_up, up, low)

    pairs = [jnp.zeros(shape, jnp.float32)] * nz
    for c, (first, last) in enumerate(bounds):
        copies[c].wait()
        for t in range(first, last):
            here = (lane == 2 * t) | (lane == (2 * t - 1) % cols)
            for k in range(nz):
                value = x_ref[pl.ds((t * nz + k) * rows, rows), :]
                pairs[k] = jnp.where(here, pltpu.roll(value, 2 * t, 1) if t else value, pairs[k])
        for t in range(first, last):
            start = t * nz * rows
            put_rows(x_ref[pl.ds(start, nz, stride=rows), :], x_ref[pl.ds(start + rows - 1, nz, stride=rows), :], t * nz)
    kmt_copy.wait()
    kmt = raw_ref[...].astype(jnp.float32)
    kmt_ref[...] = kmt
    put_rows(jnp.broadcast_to(kmt[:1], (nz, cols)), jnp.broadcast_to(kmt[rows - 1 :], (nz, cols)), nt * nz)
    for k in range(nz):
        own_ref[pl.ds(k * rows, rows), :] = pairs[k]
    for j in range(nz // per + 1):
        east = west = jnp.zeros(shape, jnp.float32)
        for i in range(per):
            k, start = j * per + i, i * nt
            if k > nz:
                break
            index = lax.rem(2 * (lane - start + cols), cols)
            if k == nz:
                side = (jnp.broadcast_to(kmt[:, cols - 1 :], shape), jnp.broadcast_to(kmt[:, :1], shape))
            else:
                side = pick(pairs[k], lax.rem(index + cols - 1, cols)), pick(pairs[k], index)
            east, west = (jnp.where(lane >= start, a, b) for a, b in zip(side, (east, west)))
        east_ref[pl.ds(j * rows, rows), :] = east
        west_ref[pl.ds(j * rows, rows), :] = west


def chunk_bounds(nt, shares):
    ends = [round(nt * share) for share in shares]
    return list(zip([0] + ends, ends))


def pairs_of(west_ref, east_ref, dims, count):
    nt, _, rows, cols, _ = dims
    per = cols // nt
    lane = lanes_of((rows, cols))
    even = lax.rem(lane, 2) == 0
    slot = jnp.where(even, lane // 2, lax.rem(lane + 1, cols) // 2)
    pairs = []
    for k in range(count):
        index = lax.rem(slot + (k % per) * nt, cols)
        part = pl.ds((k // per) * rows, rows)
        pairs.append(jnp.where(even, pick(west_ref[part, :], index), pick(east_ref[part, :], index)))
    return pairs


def early_blocks():
    odd, _, top = position()
    first = (lax.axis_index("lon") == 0) & jnp.logical_not(top)
    return tuple(jnp.where(first, jnp.where(odd, b, a), 0) for a, b in zip(EVEN, ODD))


def early_kernel(dims, x_ref, kmt_ref, *refs):
    *refs, turned_ref = refs
    early, _ = early_blocks()

    @pl.when(early > 0)
    def _():
        coefs_body(dims, x_ref, kmt_ref, *refs[2:])
        inner_body(dims, 0, early, turned_ref, x_ref, kmt_ref, *refs)


def middle_kernel(dims, x_ref, kmt_ref, *refs):
    *refs, turned_ref = refs
    refs = refs[len(refs) // 2 :]
    early, done = early_blocks()

    @pl.when((early == 0) & (done > 0))
    def _():
        coefs_body(dims, x_ref, kmt_ref, *refs[2:])

    inner_body(dims, early, done, turned_ref, x_ref, kmt_ref, *refs)


def late_kernel(dims, x_ref, kmt_ref, *refs):
    *refs, turned_ref = refs
    refs = refs[len(refs) // 2 :]
    _, done = early_blocks()

    @pl.when(done == 0)
    def _():
        coefs_body(dims, x_ref, kmt_ref, *refs[2:])

    inner_body(dims, done, dims[0] // UNROLL, turned_ref, x_ref, kmt_ref, *refs)


def coefs_body(dims, x_ref, kmt_ref, sum_y_ref, inner_ref, dense_ref, cell_w_ref, cell_e_ref, ax_ref, bx_ref, ay_ref, by_ref, p_ref, pw_ref, q_ref, z_ref):
    _, nz, rows, cols, _ = dims
    shape = (rows, cols)
    lane, row = lanes_of(shape), rows_of(shape)
    kmt = kmt_ref[...]
    heat = [x_ref[pl.ds(k * rows, rows), :] for k in range(nz)]
    salt = [x_ref[pl.ds((nz + k) * rows, rows), :] for k in range(nz)]
    density = [density_of(h, s) for h, s in zip(heat, salt)]
    wm = [as_mask(kmt > k + 1) for k in range(nz - 1)]
    kmt_w = pltpu.roll(kmt, 1, 1)
    strat = [0.5 * s for s in level_lists(density, wm)[1]]
    kmt_x = jnp.where(lane == 0, 0.0, jnp.minimum(kmt, kmt_w))
    kmt_y = jnp.where(row == 0, 0.0, jnp.minimum(kmt, pltpu.roll(kmt, 1, 0)))
    sum_x, sum_y = [], []
    for k in range(nz):
        part = pl.ds(k * rows, rows)
        mask = as_mask(kmt_x > k)
        slope = slope_at(density[k], pltpu.roll(density[k], 1, 1), mask, strat[k], pltpu.roll(strat[k], 1, 1))
        ax_ref[part, :] = REDI * mask
        bx_ref[part, :] = FACE * slope
        sum_x.append(slope + pltpu.roll(slope, cols - 1, 1))
        inner_ref[part, :] = pair_of(slope[:, 1:2], slope[:, cols - 1 :], cols)
        mask = as_mask(kmt_y > k)
        slope = slope_at(density[k], pltpu.roll(density[k], 1, 0), mask, strat[k], pltpu.roll(strat[k], 1, 0))
        ay_ref[part, :] = REDI * mask
        by_ref[part, :] = FACE * slope
        sum_y.append(slope + pltpu.roll(slope, rows - 1, 0))
        sum_y_ref[part, :] = sum_y[k]
        dense_ref[part, :] = pair_of(density[k][:, :1], density[k][:, cols - 1 :], cols)
        cell_w_ref[part, :] = jnp.zeros(shape, jnp.float32)
        cell_e_ref[part, :] = jnp.zeros(shape, jnp.float32)
    for k in range(nz - 1):
        part = pl.ds(k * rows, rows)
        level_x, level_y = 0.25 * (sum_x[k] + sum_x[k + 1]), 0.25 * (sum_y[k] + sum_y[k + 1])
        p = LEVEL * level_x * wm[k]
        p_ref[part, :] = p
        pw_ref[part, :] = pltpu.roll(p, 1, 1)
        q_ref[part, :] = LEVEL * level_y * wm[k]
        z_ref[part, :] = REDI * (level_x * level_x + level_y * level_y) * wm[k]


def inner_body(dims, first, last, turned_ref, x_ref, kmt_ref, base_ref, cy_ref, sum_y_ref, inner_ref, dense_ref, cell_w_ref, cell_e_ref,
               ax_ref, bx_ref, ay_ref, by_ref, p_ref, pw_ref, q_ref, z_ref):
    nt, nz, rows, cols, _ = dims
    lane = lanes_of((rows, cols))

    def load(ref, k):
        return ref[pl.ds(k * rows, rows), :]

    def turn(i):
        for j in range(UNROLL * nz):
            part = pl.ds(pl.multiple_of((i * UNROLL * nz + j) * rows, rows), rows)
            turned_ref[lax.rem(i, 2), pl.ds(j * rows, rows), :] = pltpu.roll(x_ref[part, :], 1, 1)

    def tracer(i, j, wm, wm_w):
        t = i * UNROLL + j
        base = t * (nz * rows)
        part = lambda k: pl.ds(pl.multiple_of(base + k * rows, rows), rows)
        value = [x_ref[part(k), :] for k in range(nz)]
        beside = [turned_ref[lax.rem(i, 2), pl.ds((j * nz + k) * rows, rows), :] for k in range(nz)]
        diff, total = level_lists(value, wm)
        total_w = level_lists(beside, wm_w)[1]
        at_east, at_west = lane == lax.rem(2 * t + cols - 1, cols), lane == 2 * t + 1
        new, grads, fluxes, cell_y = [], [], [], []
        for k in range(nz):
            grad = load(ax_ref, k) * (value[k] - beside[k])
            grads.append(grad)
            fluxes.append(grad + load(bx_ref, k) * (total[k] + total_w[k]))
            grad = load(ay_ref, k) * (value[k] - pltpu.roll(value[k], 1, 0))
            flux = grad + load(by_ref, k) * (total[k] + pltpu.roll(total[k], 1, 0))
            cell_y.append(grad + pltpu.roll(grad, rows - 1, 0))
            new.append((value[k] - fluxes[k]) + (pltpu.roll(flux, rows - 1, 0) - flux))
        down = down_w = None
        for k in range(nz):
            result, west = new[k], fluxes[k]
            if k > 0:
                result, west = result - down, west - down_w
            if k < nz - 1:
                both_x, both_y = grads[k] + grads[k + 1], cell_y[k] + cell_y[k + 1]
                down = load(p_ref, k) * both_x + load(q_ref, k) * both_y + load(z_ref, k) * diff[k]
                down_w = load(pw_ref, k) * both_x
                result, west = result + down, west + down_w
                cy_ref[part(k), :] = both_y
                moved = pltpu.roll(both_x, lax.rem(2 * t, cols), 1)
                cell_e_ref[pl.ds(k * rows, rows), :] = jnp.where(at_east, moved, load(cell_e_ref, k))
                cell_w_ref[pl.ds(k * rows, rows), :] = jnp.where(at_west, moved, load(cell_w_ref, k))
            else:
                cy_ref[part(k), :] = jnp.zeros((rows, cols), jnp.float32)
            base_ref[part(k), :] = result + pltpu.roll(west, cols - 1, 1)

    @pl.when(first < last)
    def _():
        kmt = kmt_ref[...]
        kmt_w = pltpu.roll(kmt, 1, 1)
        wm = [as_mask(kmt > k + 1) for k in range(nz - 1)]
        wm_w = [as_mask(kmt_w > k + 1) for k in range(nz - 1)]
        turn(first)

        def step(i, carry):
            for j in range(UNROLL):
                tracer(i, j, wm, wm_w)
            turn(jnp.minimum(i + 1, nt // UNROLL - 1))
            return carry

        lax.fori_loop(first, last, step, 0)


def end_kernel(color, dims, x_ref, kmt_ref, base_ref, cy_ref, sum_y_ref, there_ref, out_ref):
    nt, nz, rows, cols, _ = dims
    odd, bottom, _ = position()
    north = odd if color == 1 else jnp.logical_not(odd)
    flat = (nz, cols)
    level = rows_of(flat).astype(jnp.float32)

    def side(row, sign):
        def own_row(ref, t):
            return ref[pl.ds(t * nz * rows + row, nz, stride=rows), :]

        def ghost_row(t):
            return there_ref[pl.ds(t * nz, nz), :]

        kmts = jnp.broadcast_to(kmt_ref[row : row + 1, :], flat), ghost_row(nt)
        own_wm, ghost_wm = [as_mask(k > level + 1.0) for k in kmts]
        mask = as_mask(jnp.minimum(*kmts) > level)
        own_density = density_of(own_row(x_ref, 0), own_row(x_ref, 1))
        ghost_density = density_of(ghost_row(0), ghost_row(1))
        own_strat, ghost_strat = level_rows(own_density, own_wm)[1], level_rows(ghost_density, ghost_wm)[1]
        slope = sign * slope_at(ghost_density, own_density, mask, 0.5 * own_strat, 0.5 * ghost_strat)
        before = own_row(sum_y_ref, 0)
        before = 0.25 * (before + pltpu.roll(before, nz - 1, 0))
        change = 0.25 * (slope + pltpu.roll(slope, nz - 1, 0))
        after = before + change
        a, b = REDI * mask, sign * FACE * slope
        q, q_change = sign * LEVEL * after * own_wm, LEVEL * change * own_wm
        z_change = REDI * change * (before + after) * own_wm
        for t in range(nt):
            here, there = own_row(x_ref, t), ghost_row(t)
            diff, own_sum = level_rows(here, own_wm)
            grad = a * (there - here)
            gain = grad + b * (own_sum + level_rows(there, ghost_wm)[1])
            tilt = q * (grad + pltpu.roll(grad, nz - 1, 0)) + q_change * own_row(cy_ref, t) + z_change * diff
            part = pl.ds(t * nz * rows + row, nz, stride=rows)
            out_ref[part, :] = out_ref[part, :] + (gain + (tilt - pltpu.roll(tilt, 1, 0)))

    @pl.when(north)
    def _():
        side(rows - 1, 1.0)

    @pl.when(jnp.logical_not(north | bottom))
    def _():
        side(0, -1.0)


def outer_kernel(dims, kmt_ref, own_ref, base_ref, inner_ref, dense_ref, cell_w_ref, cell_e_ref,
                 from_west, from_east, out_hbm, out_ref, side_ref, sems):
    nt, nz, rows, cols, _ = dims
    shape = (rows, cols)
    lane = lanes_of(shape)
    per = cols // nt
    even = lax.rem(lane, 2) == 0
    kmt = kmt_ref[...]

    def load(ref, k):
        return ref[pl.ds(k * rows, rows), :]

    def spread(k, t):
        start = (k % per) * nt + t
        parts = (load(ref, k // per)[:, start : start + 1] for ref in (from_west, from_east))
        return pair_of(*parts, cols)

    outward = jnp.where(even, -1.0, 1.0)
    own = [load(own_ref, k) for k in range(nz)]
    ghost = pairs_of(from_west, from_east, dims, nz)
    own_kmt, ghost_kmt = pair_of(kmt[:, :1], kmt[:, cols - 1 :], cols), spread(nz, 0)
    own_density = [load(dense_ref, k) for k in range(nz)]
    ghost_density = [density_of(spread(k, 0), spread(k, 1)) for k in range(nz)]
    own_wm = [as_mask(own_kmt > k + 1) for k in range(nz - 1)]
    ghost_wm = [as_mask(ghost_kmt > k + 1) for k in range(nz - 1)]
    side_mask = [as_mask(jnp.minimum(own_kmt, ghost_kmt) > k) for k in range(nz)]
    own_strat = level_lists(own_density, own_wm)[1]
    ghost_strat = level_lists(ghost_density, ghost_wm)[1]
    side_slope = [
        outward * slope_at(ghost_density[k], own_density[k], side_mask[k], 0.5 * own_strat[k], 0.5 * ghost_strat[k])
        for k in range(nz)
    ]
    own_diff, own_sum = level_lists(own, own_wm)
    ghost_sum = level_lists(ghost, ghost_wm)[1]
    grad = [REDI * side_mask[k] * (ghost[k] - own[k]) for k in range(nz)]
    flux = [grad[k] + outward * FACE * side_slope[k] * (own_sum[k] + ghost_sum[k]) for k in range(nz)]
    tilt = []
    for k in range(nz - 1):
        before = 0.25 * (load(inner_ref, k) + load(inner_ref, k + 1))
        change = 0.25 * (side_slope[k] + side_slope[k + 1])
        after = before + change
        inner = jnp.where(even, pltpu.roll(load(cell_w_ref, k), cols - 1, 1), load(cell_e_ref, k))
        across = after * outward * (grad[k] + grad[k + 1]) + change * inner
        along = change * (before + after) * own_diff[k]
        tilt.append(own_wm[k] * (LEVEL * across + REDI * along))
    for k in range(nz):
        added = flux[k]
        if k < nz - 1:
            added = added + tilt[k]
        if k > 0:
            added = added - tilt[k - 1]
        side_ref[pl.ds(k * rows, rows), :] = added
    outer = (lane == 0) | (lane == cols - 1)
    copies = []
    for c, (first, last) in enumerate(chunk_bounds(nt, STORES)):
        for t in range(first, last):
            for k in range(nz):
                part = pl.ds((t * nz + k) * rows, rows)
                side = load(side_ref, k)
                side = pltpu.roll(side, cols - 2 * t, 1) if t else side
                out_ref[part, :] = base_ref[part, :] + jnp.where(outer, side, 0.0)
        part = pl.ds(first * nz * rows, (last - first) * nz * rows)
        copies.append(pltpu.make_async_copy(out_ref.at[part], out_hbm.at[part], sems.at[c]))
        copies[-1].start()
    for copy in copies:
        copy.wait()


def idle_partner(lon, lons):
    if lons % 8 == 0 and (lon * 4 // lons) % 2 == 1:
        return (lon + lons // 2) % lons
    return lon ^ 1 if lons % 2 == 0 else lon


def row_pairs(color, lons, lats):
    pairs = []
    for lon in range(lons):
        for lat in range(lats - 1):
            if lat % 2 == color:
                pairs += [(lon * lats + lat, lon * lats + lat + 1), (lon * lats + lat + 1, lon * lats + lat)]
        if (lats - 1) % 2 == color:
            pairs.append((lon * lats + lats - 1, (lons - 1 - lon) * lats + lats - 1))
    free_in = sorted(set(range(lons * lats)) - {b for _, b in pairs})
    free_out = set(range(lons * lats)) - {a for a, _ in pairs}
    for target in free_in:
        lon, lat = divmod(target, lats)
        source = idle_partner(lon, lons) * lats + lat
        assert source in free_out
        pairs.append((source, target))
    return pairs


def local(tracers, kmt):
    nt, nz, rows, cols = tracers.shape
    lons, lats = lax.axis_size("lon"), lax.axis_size("lat")
    dims = (nt, nz, rows, cols, (lats - 1) % 2)
    assert 2 * nt <= cols and nt % UNROLL == 0 and max(EVEN + ODD) <= nt // UNROLL
    packed = ((nz // (cols // nt) + 1) * rows, cols)
    edge = (nt * nz + nz, cols)
    level, block = (nz * rows, cols), (nt * nz * rows, cols)
    vmem, anywhere = pl.BlockSpec(memory_space=pltpu.VMEM), pl.BlockSpec(memory_space=pl.ANY)

    def call(kernel, inputs, out_shape, scratch, flops, specs=None, aliases={}):
        out = [pltpu.VMEM(s, jnp.float32) for s in out_shape] if specs is None else out_shape
        if specs is None:
            specs = [vmem] * len(out_shape)
        near = [pltpu.with_memory_space_constraint(a, pltpu.HBM if a is x or a is kmt else pltpu.VMEM) for a in inputs]
        return pl.pallas_call(
            functools.partial(kernel, dims),
            out_shape=out,
            in_specs=[anywhere if a is x or a is kmt else vmem for a in inputs],
            out_specs=specs,
            scratch_shapes=scratch,
            input_output_aliases=aliases,
            cost_estimate=pl.CostEstimate(flops=flops, bytes_accessed=flops, transcendentals=0),
            compiler_params=pltpu.CompilerParams(vmem_limit_bytes=16 * 2**20),
        )(*near)

    x = tracers.reshape(block)
    near, own, east, west, near_kmt, even, odd = call(
        pack_kernel,
        (x, kmt),
        (block, level, packed, packed, (rows, cols), edge, edge),
        [pltpu.VMEM((rows, cols), jnp.int32), pltpu.SemaphoreType.DMA((len(LOADS) + 1,))],
        1000000,
    )
    ring = [(i, (i + 1) % lons) for i in range(lons)]
    from_west = lax.ppermute(east, "lon", ring)
    shapes = (block,) * 2 + (level,) * 13
    turned = [pltpu.VMEM((2, UNROLL * nz * rows, cols), jnp.float32)]
    inner = call(early_kernel, (near, near_kmt), shapes, turned, 10000000)
    from_odd = lax.ppermute(odd, ("lon", "lat"), row_pairs(1, lons, lats))
    aliases = {2 + i: i for i in range(len(shapes))}
    inner = call(middle_kernel, (near, near_kmt, *inner), shapes, turned, 10000000, aliases=aliases)
    from_even = lax.ppermute(even, ("lon", "lat"), row_pairs(0, lons, lats))
    from_east = lax.ppermute(west, "lon", [(b, a) for a, b in ring])
    inner = call(late_kernel, (near, near_kmt, *inner), shapes, turned, 10000000, aliases=aliases)
    base, cy, sum_y, inner_slope, dense, cell_w, cell_e = inner[:7]
    for color, there in ((0, from_even), (1, from_odd)):
        inputs = (near, near_kmt, base, cy, sum_y, there)
        (base,) = call(functools.partial(end_kernel, color), inputs, (block,), [], 1000000, aliases={2: 0})
    out = call(
        outer_kernel,
        (near_kmt, own, base, inner_slope, dense, cell_w, cell_e, from_west, from_east),
        jax.ShapeDtypeStruct(block, jnp.float32),
        [pltpu.VMEM(block, jnp.float32), pltpu.VMEM(level, jnp.float32), pltpu.SemaphoreType.DMA((len(STORES),))],
        10000000,
        anywhere,
    )
    return out.reshape(tracers.shape)


def solution(mesh):
    return jax.shard_map(
        local,
        mesh=mesh,
        in_specs=(P(None, None, "lat", "lon"), P("lat", "lon")),
        out_specs=P(None, None, "lat", "lon"),
        check_vma=False,
    )
```
